8 devices in a mesh: frag: 1 (over z), dev: 8 (over y, x, core).
Axes of the slice: x: 2, y: 2, z: 1, core: 2. Of those that a mesh axis runs over, the one named last changes fastest.
Arguments:
- ao_ints: bfloat16 [112, 112, 112, 112], P(('frag', 'dev'))
- c_occ: bfloat16 [112, 16], P('frag')
- c_vir: bfloat16 [112, 88], P('frag')
Outputs:
- output 1: float32 [88, 88, 256], P('frag', None, 'dev')
- output 2: float32 [16, 88, 1408], P('frag', None, 'dev')
All inputs are finite; a program needn't handle non-finite values.
Results may differ from the reference program's by a relative error of at most 0.001.
Values are sent between devices in bfloat16 or wider.
A program may use at most 1 GiB of HBM per device.

```python
import jax
import jax.numpy as jnp
from jax import lax

N_AO = 112
N_OCC = 16
N_VIR = 88


def setup_inputs(seed: int = 0, part: int = 0) -> dict:
    part_key = jax.random.fold_in(jax.random.key(seed), part)
    key_ints, key_occ, key_vir = jax.random.split(part_key, 3)
    row_keys = jax.random.split(key_ints, N_AO)

    def draw_row(row_key):
        return jax.random.normal(row_key, (N_AO, N_AO, N_AO), jnp.float32).astype(jnp.bfloat16)

    ao_ints = lax.map(draw_row, row_keys)
    coef_scale = N_AO ** -0.5
    c_occ = (jax.random.normal(key_occ, (N_AO, N_OCC), jnp.float32) * coef_scale).astype(jnp.bfloat16)
    c_vir = (jax.random.normal(key_vir, (N_AO, N_VIR), jnp.float32) * coef_scale).astype(jnp.bfloat16)
    return {'ao_ints': ao_ints, 'c_occ': c_occ, 'c_vir': c_vir}


def reference(ao_ints, c_occ, c_vir):
    occ32 = c_occ.astype(jnp.float32)
    vir32 = c_vir.astype(jnp.float32)

    def first_half(ao_row):
        quarter = jnp.einsum('qrs,rx->qsx', ao_row.astype(jnp.float32), occ32).astype(jnp.bfloat16)
        quarter32 = quarter.astype(jnp.float32)
        half_oo = jnp.einsum('qsx,sj->qxj', quarter32, occ32).astype(jnp.bfloat16)
        half_ov = jnp.einsum('qsx,sb->qxb', quarter32, vir32).astype(jnp.bfloat16)
        return half_oo, half_ov

    half_oo, half_ov = lax.map(first_half, ao_ints)
    half_oo = half_oo.reshape(N_AO, N_AO, N_OCC * N_OCC).astype(jnp.float32)
    half_ov = half_ov.reshape(N_AO, N_AO, N_OCC * N_VIR).astype(jnp.float32)
    mid_oo = jnp.einsum('pqm,qb->pbm', half_oo, vir32).astype(jnp.bfloat16).astype(jnp.float32)
    mid_ov = jnp.einsum('pqm,qa->pam', half_ov, vir32).astype(jnp.bfloat16).astype(jnp.float32)
    v_abij = jnp.einsum('pa,pbm->abm', vir32, mid_oo)
    v_iajb = jnp.einsum('pi,pam->iam', occ32, mid_ov)
    return v_abij, v_iajb
```

```python
import functools

import jax
import jax.numpy as jnp
from jax import lax
from jax.experimental import pallas as pl
from jax.experimental.pallas import tpu as pltpu
from jax.sharding import PartitionSpec as P

MESH = pl.DeviceIdType.MESH
F32 = jnp.float32
BF16 = jnp.bfloat16


def dot(a, b):
    return jnp.dot(a, b, preferred_element_type=F32)


def iota(shape, d):
    return lax.broadcasted_iota(jnp.int32, shape, d)


def onehot(cond):
    return jnp.where(cond, 1.0, 0.0).astype(BF16)


def kernel(nd, np_, n, no, nv, a_ref, co_ref, cv_ref, v1_ref, v2_ref,
           a_buf, t_buf, w_buf, cot, cvt, s_buf, r_buf, l1_buf, l2_buf,
           a_sem, send_sem, recv_sem):
    me = lax.axis_index("dev")
    frag = lax.axis_index("frag")
    nab = nv // 8

    def a_copy(p):
        slot = lax.rem(p, 2)
        return pltpu.make_async_copy(a_ref.at[p], a_buf.at[slot], a_sem.at[slot])

    a_copy(0).start()

    barrier = pltpu.get_barrier_semaphore()
    for k in range(1, nd):
        pl.semaphore_signal(barrier, inc=1, device_id=(frag, lax.rem(me + k, nd)), device_id_type=MESH)

    co = co_ref[...]
    cv = cv_ref[...]
    eye = onehot(iota((n, n), 0) == iota((n, n), 1))
    tdims = (((0,), (0,)), ((), ()))
    cot[...] = lax.dot_general(co, eye, tdims, preferred_element_type=F32).astype(BF16)
    cvt[...] = lax.dot_general(cv, eye, tdims, preferred_element_type=F32).astype(BF16)
    w_buf[...] = jnp.zeros_like(w_buf)
    t_buf[...] = jnp.zeros_like(t_buf)
    for j in range(2):
        b = iota((nv, 256), 0) + j * nv
        c = iota((nv, 256), 1)
        sel_v = onehot(c == jnp.where(b < 128, b, b + 32))
        jj = iota((no, 256), 0) + 128 + no * j
        sel_o = onehot(iota((no, 256), 1) == jj)
        w_buf[128 * j:128 * j + n, :] = (dot(cv, sel_v) + dot(co, sel_o)).astype(BF16)

    pl.semaphore_wait(barrier, nd - 1)

    def remote(p, k):
        d = lax.rem(me + k, nd)
        return pltpu.make_async_remote_copy(
            src_ref=s_buf.at[p, k], dst_ref=r_buf.at[p, me],
            send_sem=send_sem.at[p, k], recv_sem=recv_sem.at[p, me],
            device_id=(frag, d), device_id_type=MESH)

    def row(p, _):
        slot = lax.rem(p, 2)
        a_copy(p).wait()

        @pl.when(p + 1 < np_)
        def _():
            a_copy(p + 1).start()

        UQ = 8

        def step1(g, _):
            for u in range(UQ):
                q = g * UQ + u
                t = dot(cot[...], a_buf[slot, q])
                t_buf[pl.ds(q * no, no), 0:n] = t
            return 0

        lax.fori_loop(0, n // UQ, step1, 0)

        def step23(k):
            d = lax.rem(me + k, nd)
            t0 = t_buf[pl.ds(2 * d, n, stride=no), :].astype(BF16)
            t1 = t_buf[pl.ds(2 * d + 1, n, stride=no), :].astype(BF16)
            h = dot(jnp.concatenate([t0, t1], axis=1), w_buf[...]).astype(BF16)
            return dot(cvt[...], h).astype(BF16).reshape(nab, 8, 256)

        def dest(k, _):
            s_buf[p, k] = step23(k)
            remote(p, k).start()
            return 0

        lax.fori_loop(1, nd, dest, 0)
        r_buf[p, me] = step23(0)
        return 0

    lax.fori_loop(0, np_, row, 0)

    PB = 4
    for lo in range(0, np_, PB):
        pb = min(PB, np_ - lo)
        kk = pb * nd * 8
        k_i = iota((n, kk), 1)
        perm = onehot(iota((n, kk), 0) == np_ * ((k_i // 8) % nd) + lo + k_i // (8 * nd))
        for m, tab, out in ((no, cot, l2_buf), (nv, cvt, l1_buf)):
            rep = onehot(iota((m * 8, m), 0) // 8 == iota((m * 8, m), 1))
            x = dot(tab[...], perm).astype(BF16)
            x = dot(rep, x)
            same = (iota((m * 8, kk), 0) % 8) == (iota((m * 8, kk), 1) % 8)
            out[:, 0:kk] = jnp.where(same, x, 0.0).astype(BF16)

        def wait_one(idx, _):
            p = lo + idx // (nd - 1)
            src = lax.rem(me + 1 + lax.rem(idx, nd - 1), nd)
            pltpu.make_async_remote_copy(
                src_ref=s_buf.at[p, 1], dst_ref=r_buf.at[p, src],
                send_sem=send_sem.at[p, 1], recv_sem=recv_sem.at[p, src],
                device_id=(frag, src), device_id_type=MESH).wait_recv()
            return 0

        lax.fori_loop(0, pb * (nd - 1), wait_one, 0)

        def block(ab, _):
            r = r_buf[lo:lo + pb, :, ab].reshape(kk, 256)
            o2 = dot(l2_buf[:, 0:kk], r).reshape(no, 8, 256)
            o1 = dot(l1_buf[:, 0:kk], r[:, 128:256]).reshape(nv, 8, 128)
            rows = pl.ds(pl.multiple_of(ab * 8, 8), 8)
            if lo == 0:
                v2_ref[:, rows, 0:128] = o2[:, :, 0:128]
                v2_ref[:, rows, 128:176] = o2[:, :, 160:208]
                v1_ref[:, rows, :] = o1[:, :, 0:32]
            else:
                v2_ref[:, rows, 0:128] += o2[:, :, 0:128]
                v2_ref[:, rows, 128:176] += o2[:, :, 160:208]
                v1_ref[:, rows, :] += o1[:, :, 0:32]
            return 0

        lax.fori_loop(0, nab, block, 0)

    def drain(idx, _):
        p = idx // (nd - 1)
        k = 1 + lax.rem(idx, nd - 1)
        remote(p, k).wait_send()
        return 0

    lax.fori_loop(0, np_ * (nd - 1), drain, 0)


def solution(mesh):
    nd = mesh.shape["dev"]

    def local_part(a, co, cv):
        np_, n = a.shape[0], a.shape[1]
        no, nv = co.shape[1], cv.shape[1]
        vm = pl.BlockSpec(memory_space=pltpu.VMEM)
        return pl.pallas_call(
            functools.partial(kernel, nd, np_, n, no, nv),
            out_shape=(jax.ShapeDtypeStruct((nv, nv, no * no // nd), F32),
                       jax.ShapeDtypeStruct((no, nv, no * nv // nd), F32)),
            in_specs=[pl.BlockSpec(memory_space=pl.ANY), vm, vm],
            out_specs=(vm, vm),
            scratch_shapes=[
                pltpu.VMEM((2, n, n, n), BF16),
                pltpu.VMEM((n * no, 128), F32),
                pltpu.VMEM((256, 256), BF16),
                pltpu.VMEM((no, n), BF16),
                pltpu.VMEM((nv, n), BF16),
                pltpu.VMEM((np_, nd, nv // 8, 8, 256), BF16),
                pltpu.VMEM((np_, nd, nv // 8, 8, 256), BF16),
                pltpu.VMEM((nv * 8, 256), BF16),
                pltpu.VMEM((no * 8, 256), BF16),
                pltpu.SemaphoreType.DMA((2,)),
                pltpu.SemaphoreType.DMA((np_, nd)),
                pltpu.SemaphoreType.DMA((np_, nd)),
            ],
            compiler_params=pltpu.CompilerParams(
                collective_id=0, has_side_effects=True, vmem_limit_bytes=60 * 1024 * 1024),
        )(a, co, cv)

    return jax.shard_map(local_part, mesh=mesh,
                         in_specs=(P(('frag', 'dev')), P('frag'), P('frag')),
                         out_specs=(P('frag', None, 'dev'), P('frag', None, 'dev')),
                         check_vma=False)
```

```python
import functools

import jax
import jax.numpy as jnp
from jax import lax
from jax.experimental import pallas as pl
from jax.experimental.pallas import tpu as pltpu
from jax.sharding import PartitionSpec as P

MESH = pl.DeviceIdType.MESH
F32 = jnp.float32
BF16 = jnp.bfloat16
NX = 6
LAG = 3


def dot(a, b):
    return jnp.dot(a, b, preferred_element_type=F32)


def dot_t(a, b):
    return lax.dot_general(a, b, (((0,), (0,)), ((), ())), preferred_element_type=F32)


def iota(shape, d):
    return lax.broadcasted_iota(jnp.int32, shape, d)


def onehot(cond):
    return jnp.where(cond, 1.0, 0.0).astype(BF16)


def kernel(np_, n, no, nv, a_ref, cot_ref, cvt_ref, v1_ref, v2_ref,
           a_buf, la, ww, cv_buf, t_buf, h_buf, lx, ly, l1,
           sx, sy, so, rx, ry, ro, px, py, qx, qy,
           a_sem, sx_sem, sy_sem, so_sem, rx_sem, ry_sem, ro_sem,
           px_sem, py_sem, qx_sem, qy_sem):
    nd = 8
    npair = np_ // 2
    nb = nv // 8
    NY = nb - NX
    ng = n // 16
    me = lax.axis_index("dev")
    frag = lax.axis_index("frag")
    y, x, c = me // 4, (me // 2) % 2, me % 2

    def dev(k):
        dy, dx, dc = k
        return (1 - y if dy else y) * 4 + (1 - x if dx else x) * 2 + (1 - c if dc else c)

    def did(k):
        return (frag, dev(k))

    KS = [(1, 1, 0), (1, 1, 1), (1, 0, 1), (0, 1, 1), (1, 0, 0), (0, 1, 0), (0, 0, 1), (0, 0, 0)]

    def a_copy(p, g):
        slot = p % 4
        return pltpu.make_async_copy(a_ref.at[p, pl.ds(16 * g, 16)], a_buf.at[slot, pl.ds(16 * g, 16)],
                                     a_sem.at[slot, g])

    for p in range(2):
        for g in range(ng):
            a_copy(p, g).start()

    barrier = pltpu.get_barrier_semaphore()
    for k in KS[:-1]:
        pl.semaphore_signal(barrier, inc=1, device_id=did(k), device_id_type=MESH)

    cot = cot_ref[...]
    cvt = cvt_ref[...]
    co = dot_t(cot, onehot(iota((no, no), 0) == iota((no, no), 1))).astype(BF16)
    cv = dot_t(cvt, onehot(iota((nv, nv), 0) == iota((nv, nv), 1))).astype(BF16)
    cv_buf[...] = cv
    rep8 = onehot(iota((no * 8, no), 0) // 8 == iota((no * 8, no), 1))
    tile = onehot(iota((n, 8 * n), 0) == iota((n, 8 * n), 1) % n)
    m = dot(rep8, dot(cot, tile).astype(BF16))
    la[...] = jnp.where(iota(m.shape, 0) % 8 == iota(m.shape, 1) // n, m, 0.0).astype(BF16)
    ww[...] = jnp.zeros_like(ww)
    for par in range(2):
        for j in range(2):
            jb = iota((nv, 512), 0) + j * nv
            col = iota((nv, 512), 1)
            sel_v = onehot(col == jnp.where(jb < 128, par * 128 + jb, 256 + 48 * par + jb - 128))
            sel_o = onehot(iota((no, 512), 1) == iota((no, 512), 0) + 384 + 32 * par + no * j)
            r0 = 256 * par + 128 * j
            ww[r0:r0 + n, :] = (dot(cv, sel_v) + dot(co, sel_o)).astype(BF16)

    for p in range(2, 4):
        for g in range(ng):
            a_copy(p, g).start()

    def kron(tab, m_, kk, p_of_col, same):
        perm = onehot(iota((n, kk), 0) == p_of_col(iota((n, kk), 1)))
        r = onehot(iota((m_ * 8, m_), 0) // 8 == iota((m_ * 8, m_), 1))
        v = dot(r, dot(tab, perm).astype(BF16))
        return jnp.where(iota(v.shape, 0) % 8 == same(iota(v.shape, 1)), v, 0.0).astype(BF16)

    k4 = npair * 32
    for par in range(2):
        lx[par] = kron(cot, no, k4, lambda t: np_ * (y * 4 + (t // 8) % 4) + 2 * (t // 32) + par, lambda t: t % 8)
        ly[par] = kron(cot, no, k4, lambda t: np_ * ((t // 16) % 2 * 4 + x * 2 + (t // 8) % 2) + 2 * (t // 32) + par,
                       lambda t: t % 8)

    pl.semaphore_wait(barrier, nd - 1)

    def send_x(i, k):
        h = (0, k[1], k[2])
        return pltpu.make_async_remote_copy(
            src_ref=sx.at[i, dev(k)], dst_ref=rx.at[i, x * 2 + c, k[0]],
            send_sem=sx_sem.at[i, dev(k)], recv_sem=rx_sem.at[i, x * 2 + c, k[0]],
            device_id=did(h), device_id_type=MESH)

    def send_y(i, k):
        h = (k[0], 0, k[2])
        return pltpu.make_async_remote_copy(
            src_ref=sy.at[i, dev(k)], dst_ref=ry.at[i, y * 2 + c, k[1]],
            send_sem=sy_sem.at[i, dev(k)], recv_sem=ry_sem.at[i, y * 2 + c, k[1]],
            device_id=did(h), device_id_type=MESH)

    def send_o(i, k):
        return pltpu.make_async_remote_copy(
            src_ref=so.at[i, dev(k)], dst_ref=ro.at[i, me],
            send_sem=so_sem.at[i, dev(k)], recv_sem=ro_sem.at[i, me],
            device_id=did(k), device_id_type=MESH)

    def far_x(k):
        return bool(k[1] or k[2])

    def far_y(k):
        return bool(k[0] or k[2])

    def send_relay(i):
        for k in KS:
            if far_x(k) and k[0]:
                send_x(i, k).start()
            if far_y(k) and k[1]:
                send_y(i, k).start()

    def send_direct(i):
        for k in KS:
            if far_x(k) and not k[0]:
                send_x(i, k).start()
            if far_y(k) and not k[1]:
                send_y(i, k).start()
            if k != (0, 0, 0):
                send_o(i, k).start()

    zpad = jnp.zeros((8 * n, 128 - n), BF16)

    def pair(i, _):
        for par in range(2):
            p = 2 * i + par
            slot = p % 4

            def step1(g, _):
                a_copy(p, g).wait()
                a0 = a_buf[slot, pl.ds(16 * g, 8)].reshape(8 * n, n)
                a1 = a_buf[slot, pl.ds(16 * g + 8, 8)].reshape(8 * n, n)
                w = jnp.concatenate([a0, zpad, a1, zpad], axis=1)
                t = dot(la[...], w)
                rows = pl.ds(pl.multiple_of(16 * g, 16), 16)
                for xx in range(no):
                    tx = t[8 * xx:8 * xx + 8]
                    tx = jnp.concatenate([tx[:, 0:128], tx[:, 128:256]], axis=0).astype(BF16)
                    l0 = par * 256 + (xx % 2) * 128
                    t_buf[xx // 2, rows, l0:l0 + 128] = tx
                return 0

            lax.fori_loop(0, ng, step1, 0)

            @pl.when(p + 4 < np_)
            def _():
                for g in range(ng):
                    a_copy(p + 4, g).start()

        def step2(d, _):
            tt = t_buf[pl.ds(4 * d, 4)].reshape(4 * n, 512)
            h_buf[pl.ds(4 * d, 4)] = dot(tt, ww[...]).astype(BF16).reshape(4, n, 512)
            return 0

        lax.fori_loop(0, 2, step2, 0)

        for k in KS:
            d = dev(k)
            h = h_buf[d]
            g = dot(cvt_ref[...], h[:, 0:384]).astype(BF16).reshape(nb, 8, 384)
            if far_x(k):
                sx[i, d] = g[0:NX]
            else:
                rx[i, x * 2 + c, k[0]] = g[0:NX]
            if far_y(k):
                sy[i, d] = g[NX:nb]
            else:
                ry[i, y * 2 + c, k[1]] = g[NX:nb]
            go = dot_t(h[:, 384:384 + 4 * no], cv_buf[...]).astype(BF16)
            if k == (0, 0, 0):
                ro[i, me] = go
            else:
                so[i, d] = go

        send_relay(i)

        @pl.when(i >= LAG)
        def _():
            send_direct(i - LAG)

        return 0

    lax.fori_loop(0, npair, pair, 0)
    for i in range(npair - LAG, npair):
        send_direct(i)

    def wait_x(i, sc, w):
        pltpu.make_async_remote_copy(
            src_ref=rx.at[i, sc, w], dst_ref=rx.at[i, sc, w], send_sem=sx_sem.at[0, 0],
            recv_sem=rx_sem.at[i, sc, w], device_id=did((0, 0, 1)), device_id_type=MESH).wait_recv()

    def wait_y(i, sc, w):
        pltpu.make_async_remote_copy(
            src_ref=ry.at[i, sc, w], dst_ref=ry.at[i, sc, w], send_sem=sy_sem.at[0, 0],
            recv_sem=ry_sem.at[i, sc, w], device_id=did((0, 0, 1)), device_id_type=MESH).wait_recv()

    def wait_o(i, src):
        pltpu.make_async_remote_copy(
            src_ref=ro.at[i, src], dst_ref=ro.at[i, src], send_sem=so_sem.at[0, 0],
            recv_sem=ro_sem.at[i, src], device_id=did((0, 0, 1)), device_id_type=MESH).wait_recv()

    def wait_v2(w):
        def body(i, _):
            for e in range(1, 4):
                wait_x(i, (x * 2 + c + e) % 4, w)
                wait_y(i, (y * 2 + c + e) % 4, w)
            return 0
        lax.fori_loop(0, npair, body, 0)

    def partial(r, left, w, ab):
        v = r[:, :, w, ab].reshape(k4, 384)
        main = dot(left[0], v[:, 0:128]) + dot(left[1], v[:, 128:256])
        even = dot(left[0], v[:, 256:384])
        odd = dot(left[1], v[:, 256:384])
        return main.reshape(no, 8, 128), even.reshape(no, 8, 128), odd.reshape(no, 8, 128)

    lane = iota((8, 8, 128), 2)

    def send_p(buf, out, ssem, rsem, h, ab):
        return pltpu.make_async_remote_copy(
            src_ref=buf.at[ab], dst_ref=out.at[ab], send_sem=ssem.at[ab], recv_sem=rsem.at[ab],
            device_id=did(h), device_id_type=MESH)

    wait_v2(1)
    for r, left, buf, out, ssem, rsem, h, cnt in (
            (rx, lx, px, qx, px_sem, qx_sem, (1, 0, 0), NX), (ry, ly, py, qy, py_sem, qy_sem, (0, 1, 0), NY)):
        def relay(ab, _, r=r, left=left, buf=buf, out=out, ssem=ssem, rsem=rsem, h=h):
            main, even, odd = partial(r, left, 1, ab)
            buf[ab, 0:no] = main
            lo = even[0:8] + pltpu.roll(odd[0:8], 80, 2)
            hi = pltpu.roll(even[8:16], 48, 2) + odd[8:16]
            buf[ab, no:no + 8] = jnp.where(lane < 48, lo, hi)
            send_p(buf, out, ssem, rsem, h, ab).start()
            return 0
        lax.fori_loop(0, cnt, relay, 0)

    wait_v2(0)
    for r, left, cnt, base in ((rx, lx, NX, 0), (ry, ly, NY, NX)):
        def own(ab, _, r=r, left=left, base=base):
            main, even, odd = partial(r, left, 0, ab)
            rows = pl.ds(pl.multiple_of((ab + base) * 8, 8), 8)
            v2_ref[:, rows, 0:128] = main
            v2_ref[:, rows, 128:176] = (even + pltpu.roll(odd, 80, 2))[:, :, 0:48]
            return 0
        lax.fori_loop(0, cnt, own, 0)

    k8 = npair * 128
    l1[...] = kron(cvt_ref[...], nv, k8,
                   lambda t: np_ * ((t // 16) % 8) + 2 * (t // 128) + (t // 8) % 2, lambda t: t % 8)

    def wait_oo(i, _):
        for e in range(1, nd):
            wait_o(i, (me + e) % nd)
        return 0
    lax.fori_loop(0, npair, wait_oo, 0)

    for ib in range(4):
        def oo_rows(par):
            return ro[:, :, par * 32 + 8 * ib:par * 32 + 8 * ib + 8].reshape(npair * nd, 8, nv)
        w = jnp.concatenate([oo_rows(0), oo_rows(1)], axis=1).reshape(k8, nv)
        v1_ref[:, 8 * ib:8 * ib + 8, :] = dot(l1[...], w).reshape(nv, 8, nv)

    for buf, out, ssem, rsem, h, cnt, base in (
            (px, qx, px_sem, qx_sem, (1, 0, 0), NX, 0), (py, qy, py_sem, qy_sem, (0, 1, 0), NY, NX)):
        def add(ab, _, buf=buf, out=out, ssem=ssem, rsem=rsem, h=h, base=base):
            send_p(buf, out, ssem, rsem, h, ab).wait()
            rows = pl.ds(pl.multiple_of((ab + base) * 8, 8), 8)
            v2_ref[:, rows, 0:128] += out[ab, 0:no]
            ext = out[ab, no:no + 8]
            v2_ref[0:8, rows, 128:176] += ext[:, :, 0:48]
            v2_ref[8:16, rows, 128:176] += pltpu.roll(ext, 80, 2)[:, :, 0:48]
            return 0
        lax.fori_loop(0, cnt, add, 0)

    def drain(i, _):
        for k in KS:
            if far_x(k):
                send_x(i, k).wait_send()
            if far_y(k):
                send_y(i, k).wait_send()
            if k != (0, 0, 0):
                send_o(i, k).wait_send()
        return 0
    lax.fori_loop(0, npair, drain, 0)


def solution(mesh):
    nd = mesh.shape["dev"]

    def local_part(a, co, cv):
        np_, n = a.shape[0], a.shape[1]
        no, nv = co.shape[1], cv.shape[1]
        npair, nb = np_ // 2, nv // 8
        ny = nb - NX
        vm = pl.BlockSpec(memory_space=pltpu.VMEM)
        dma = pltpu.SemaphoreType.DMA
        v1, v2 = pl.pallas_call(
            functools.partial(kernel, np_, n, no, nv),
            out_shape=(jax.ShapeDtypeStruct((nv, no * no // nd, nv), F32),
                       jax.ShapeDtypeStruct((no, nv, no * nv // nd), F32)),
            in_specs=[pl.BlockSpec(memory_space=pl.ANY), vm, vm],
            out_specs=(vm, vm),
            scratch_shapes=[
                pltpu.VMEM((4, n, n, n), BF16),
                pltpu.VMEM((no * 8, n * 8), BF16),
                pltpu.VMEM((512, 512), BF16),
                pltpu.VMEM((n, nv), BF16),
                pltpu.VMEM((nd, n, 512), BF16),
                pltpu.VMEM((nd, n, 512), BF16),
                pltpu.VMEM((2, no * 8, npair * 32), BF16),
                pltpu.VMEM((2, no * 8, npair * 32), BF16),
                pltpu.VMEM((nv * 8, npair * 128), BF16),
                pltpu.VMEM((npair, nd, NX, 8, 384), BF16),
                pltpu.VMEM((npair, nd, ny, 8, 384), BF16),
                pltpu.VMEM((npair, nd, 4 * no, nv), BF16),
                pltpu.VMEM((npair, 4, 2, NX, 8, 384), BF16),
                pltpu.VMEM((npair, 4, 2, ny, 8, 384), BF16),
                pltpu.VMEM((npair, nd, 4 * no, nv), BF16),
                pltpu.VMEM((NX, no + 8, 8, 128), F32),
                pltpu.VMEM((ny, no + 8, 8, 128), F32),
                pltpu.VMEM((NX, no + 8, 8, 128), F32),
                pltpu.VMEM((ny, no + 8, 8, 128), F32),
                dma((4, n // 16)),
                dma((npair, nd)), dma((npair, nd)), dma((npair, nd)),
                dma((npair, 4, 2)), dma((npair, 4, 2)), dma((npair, nd)),
                dma((NX,)), dma((ny,)), dma((NX,)), dma((ny,)),
            ],
            compiler_params=pltpu.CompilerParams(
                collective_id=0, has_side_effects=True, vmem_limit_bytes=60 * 1024 * 1024),
        )(a, co.T, cv.T)
        return v1.transpose(0, 2, 1), v2

    return jax.shard_map(local_part, mesh=mesh,
                         in_specs=(P(('frag', 'dev')), P('frag'), P('frag')),
                         out_specs=(P('frag', None, 'dev'), P('frag', None, 'dev')),
                         check_vma=False)
```

```python
import functools

import jax
import jax.numpy as jnp
from jax import lax
from jax.experimental import pallas as pl
from jax.experimental.pallas import tpu as pltpu
from jax.sharding import PartitionSpec as P

MESH = pl.DeviceIdType.MESH
F32 = jnp.float32
BF16 = jnp.bfloat16
NX = 6
LAG = 1


def dot(a, b):
    return jnp.dot(a, b, preferred_element_type=F32)


def dot_t(a, b):
    return lax.dot_general(a, b, (((0,), (0,)), ((), ())), preferred_element_type=F32)


def iota(shape, d):
    return lax.broadcasted_iota(jnp.int32, shape, d)


def onehot(cond):
    return jnp.where(cond, 1.0, 0.0).astype(BF16)


def kernel(np_, n, no, nv, a_ref, cot_ref, cvt_ref, v1_ref, v2_ref,
           a_buf, la, ww, cv_buf, t_buf, h_buf, lx, ly, l1,
           sx, sy, so, sp, rx, ry, rp, ro, px, py, qx, qy,
           a_sem, s_sem, rx_sem, ry_sem, ro_sem, p_sem, qx_sem, qy_sem):
    nd = 8
    npair = np_ // 2
    nb = nv // 8
    NY = nb - NX
    ng = n // 16
    me = lax.axis_index("dev")
    frag = lax.axis_index("frag")
    y, x, c = me // 4, (me // 2) % 2, me % 2

    def dev(k):
        dy, dx, dc = k
        return (1 - y if dy else y) * 4 + (1 - x if dx else x) * 2 + (1 - c if dc else c)

    def did(k):
        return (frag, dev(k))

    KS = [(1, 1, 0), (1, 1, 1), (1, 0, 1), (0, 1, 1), (1, 0, 0), (0, 1, 0), (0, 0, 1), (0, 0, 0)]

    def a_copy(p, g):
        slot = p % 4
        return pltpu.make_async_copy(a_ref.at[p, pl.ds(16 * g, 16)], a_buf.at[slot, pl.ds(16 * g, 16)],
                                     a_sem.at[slot])

    for p in range(2):
        for g in range(ng):
            a_copy(p, g).start()

    barrier = pltpu.get_barrier_semaphore()
    for k in KS[:-1]:
        pl.semaphore_signal(barrier, inc=1, device_id=did(k), device_id_type=MESH)

    cot = cot_ref[...]
    cvt = cvt_ref[...]
    co = dot_t(cot, onehot(iota((no, no), 0) == iota((no, no), 1))).astype(BF16)
    cv = dot_t(cvt, onehot(iota((nv, nv), 0) == iota((nv, nv), 1))).astype(BF16)
    cv_buf[...] = cv
    rep8 = onehot(iota((no * 8, no), 0) // 8 == iota((no * 8, no), 1))
    tile = onehot(iota((n, 8 * n), 0) == iota((n, 8 * n), 1) % n)
    m = dot(rep8, dot(cot, tile).astype(BF16))
    la[...] = jnp.where(iota(m.shape, 0) % 8 == iota(m.shape, 1) // n, m, 0.0).astype(BF16)
    ww[...] = jnp.zeros_like(ww)
    for par in range(2):
        for j in range(2):
            jb = iota((nv, 512), 0) + j * nv
            col = iota((nv, 512), 1)
            sel_v = onehot(col == jnp.where(jb < 128, par * 128 + jb, 256 + 48 * par + jb - 128))
            sel_o = onehot(iota((no, 512), 1) == iota((no, 512), 0) + 384 + 32 * par + no * j)
            r0 = 256 * par + 128 * j
            ww[r0:r0 + n, :] = (dot(cv, sel_v) + dot(co, sel_o)).astype(BF16)

    for p in range(2, 4):
        for g in range(ng):
            a_copy(p, g).start()

    def kron(tab, m_, kk, p_of_col, same):
        perm = onehot(iota((n, kk), 0) == p_of_col(iota((n, kk), 1)))
        r = onehot(iota((m_ * 8, m_), 0) // 8 == iota((m_ * 8, m_), 1))
        v = dot(r, dot(tab, perm).astype(BF16))
        return jnp.where(iota(v.shape, 0) % 8 == same(iota(v.shape, 1)), v, 0.0).astype(BF16)

    def send_x(i, k):
        h = (0, k[1], k[2])
        return pltpu.make_async_remote_copy(
            src_ref=sx.at[dev(k), i], dst_ref=rx.at[k[0], x * 2 + c, i],
            send_sem=s_sem.at[0], recv_sem=rx_sem.at[k[0]], device_id=did(h), device_id_type=MESH)

    def send_y(i, k):
        h = (k[0], 0, k[2])
        return pltpu.make_async_remote_copy(
            src_ref=sy.at[dev(k), i], dst_ref=ry.at[k[1], y * 2 + c, i],
            send_sem=s_sem.at[1], recv_sem=ry_sem.at[k[1]], device_id=did(h), device_id_type=MESH)

    def send_o(k):
        return pltpu.make_async_remote_copy(
            src_ref=sp.at[dev(k)], dst_ref=rp.at[me],
            send_sem=s_sem.at[2], recv_sem=ro_sem, device_id=did(k), device_id_type=MESH)

    def far_x(k):
        return bool(k[1] or k[2])

    def far_y(k):
        return bool(k[0] or k[2])

    def send_relay(i, k):
        if far_x(k) and k[0]:
            send_x(i, k).start()
        if far_y(k) and k[1]:
            send_y(i, k).start()

    def send_direct(i):
        for k in KS:
            if far_x(k) and not k[0]:
                send_x(i, k).start()
            if far_y(k) and not k[1]:
                send_y(i, k).start()

    zpad = jnp.zeros((8 * n, 128 - n), BF16)

    def pair(i, _):
        for par in range(2):
            p = 2 * i + par
            slot = p % 4

            pltpu.make_async_copy(a_ref.at[p], a_buf.at[slot], a_sem.at[slot]).wait()
            for g in range(ng):
                a0 = a_buf[slot, 16 * g:16 * g + 8].reshape(8 * n, n)
                a1 = a_buf[slot, 16 * g + 8:16 * g + 16].reshape(8 * n, n)
                w = jnp.concatenate([a0, zpad, a1, zpad], axis=1)
                t = dot(la[...], w)
                for xx in range(no):
                    tx = t[8 * xx:8 * xx + 8]
                    tx = jnp.concatenate([tx[:, 0:128], tx[:, 128:256]], axis=0).astype(BF16)
                    l0 = par * 256 + (xx % 2) * 128
                    t_buf[xx // 2, 16 * g:16 * g + 16, l0:l0 + 128] = tx

            @pl.when(p + 4 < np_)
            def _():
                for g in range(ng):
                    a_copy(p + 4, g).start()

        def step2(d, _):
            tt = t_buf[pl.ds(4 * d, 4)].reshape(4 * n, 512)
            h_buf[pl.ds(4 * d, 4)] = dot(tt, ww[...]).astype(BF16).reshape(4, n, 512)
            return 0

        lax.fori_loop(0, 2, step2, 0)

        for kn, k in enumerate(KS):
            d = dev(k)
            h = h_buf[d]
            g = dot(cvt_ref[...], h[:, 0:384]).astype(BF16).reshape(nb, 8, 384)
            if far_x(k):
                sx[d, i] = g[0:NX]
            else:
                rx[k[0], x * 2 + c, i] = g[0:NX]
            if far_y(k):
                sy[d, i] = g[NX:nb]
            else:
                ry[k[1], y * 2 + c, i] = g[NX:nb]
            so[d, i] = dot_t(h[:, 384:384 + 4 * no], cv_buf[...]).astype(BF16)
            if kn == 1:
                @pl.when(i == 0)
                def _():
                    pl.semaphore_wait(barrier, nd - 1)
            if kn > 0:
                send_relay(i, KS[kn - 1])

        @pl.when(i >= LAG)
        def _():
            send_direct(i - LAG)

        return 0

    lax.fori_loop(0, npair, pair, 0)
    for i in range(npair - LAG, npair):
        send_direct(i)

    def pack(d, _):
        sp[d, :, 0:npair * nv] = jnp.concatenate([so[d, i] for i in range(npair)], axis=1)
        return 0
    lax.fori_loop(0, nd, pack, 0)
    rp[me] = sp[me]
    for k in KS[:-1]:
        send_o(k).start()

    k4 = npair * 32
    for par in range(2):
        lx[par] = kron(cot, no, k4, lambda t: np_ * (y * 4 + t // (8 * npair)) + 2 * ((t // 8) % npair) + par,
                       lambda t: t % 8)
        ly[par] = kron(cot, no, k4, lambda t: np_ * (t // (16 * npair) * 4 + x * 2 + t // (8 * npair) % 2) + 2 * ((t // 8) % npair) + par,
                       lambda t: t % 8)

    def wait_recv(buf, sem):
        pltpu.make_async_remote_copy(
            src_ref=buf, dst_ref=buf, send_sem=s_sem.at[0], recv_sem=sem,
            device_id=did((0, 0, 1)), device_id_type=MESH).wait_recv()

    def wait_send(buf, sem):
        pltpu.make_async_remote_copy(
            src_ref=buf, dst_ref=buf, send_sem=sem, recv_sem=ro_sem,
            device_id=did((0, 0, 1)), device_id_type=MESH).wait_send()

    def wait_v2(w):
        wait_recv(rx.at[w, pl.ds(0, 3)], rx_sem.at[w])
        wait_recv(ry.at[w, pl.ds(0, 3)], ry_sem.at[w])

    def partial(r, left, w, ab):
        v = r[w, :, :, ab].reshape(k4, 384)
        main = dot(left[0], v[:, 0:128]) + dot(left[1], v[:, 128:256])
        even = dot(left[0], v[:, 256:384])
        odd = dot(left[1], v[:, 256:384])
        return main.reshape(no, 8, 128), even.reshape(no, 8, 128), odd.reshape(no, 8, 128)

    lane = iota((8, 8, 128), 2)

    def send_p(buf, out, ssem, rsem, h, ab):
        return pltpu.make_async_remote_copy(
            src_ref=buf.at[ab], dst_ref=out.at[ab], send_sem=ssem, recv_sem=rsem.at[ab],
            device_id=did(h), device_id_type=MESH)

    wait_v2(1)
    for r, left, buf, out, ssem, rsem, h, cnt in (
            (rx, lx, px, qx, p_sem.at[0], qx_sem, (1, 0, 0), NX), (ry, ly, py, qy, p_sem.at[1], qy_sem, (0, 1, 0), NY)):
        def relay(ab, _, r=r, left=left, buf=buf, out=out, ssem=ssem, rsem=rsem, h=h):
            main, even, odd = partial(r, left, 1, ab)
            buf[ab, 0:no] = main
            lo = even[0:8] + pltpu.roll(odd[0:8], 80, 2)
            hi = pltpu.roll(even[8:16], 48, 2) + odd[8:16]
            buf[ab, no:no + 8] = jnp.where(lane < 48, lo, hi)
            send_p(buf, out, ssem, rsem, h, ab).start()
            return 0
        lax.fori_loop(0, cnt, relay, 0)

    wait_v2(0)
    for r, left, cnt, base in ((rx, lx, NX, 0), (ry, ly, NY, NX)):
        def own(ab, _, r=r, left=left, base=base):
            main, even, odd = partial(r, left, 0, ab)
            rows = pl.ds(pl.multiple_of((ab + base) * 8, 8), 8)
            v2_ref[:, rows, 0:128] = main
            v2_ref[:, rows, 128:176] = (even + pltpu.roll(odd, 80, 2))[:, :, 0:48]
            return 0
        lax.fori_loop(0, cnt, own, 0)

    k8 = npair * 128
    l1[...] = kron(cvt_ref[...], nv, k8,
                   lambda t: np_ * (t // (16 * npair)) + 2 * ((t // 16) % npair) + (t // 8) % 2,
                   lambda t: t % 8)

    wait_recv(rp.at[pl.ds(0, nd - 1)], ro_sem)

    def unpack(d, _):
        v = rp[d]
        for i in range(npair):
            ro[d, i] = v[:, nv * i:nv * i + nv]
        return 0
    lax.fori_loop(0, nd, unpack, 0)

    for ib in range(4):
        def oo_rows(par):
            return ro[:, :, par * 32 + 8 * ib:par * 32 + 8 * ib + 8].reshape(npair * nd, 8, nv)
        w = jnp.concatenate([oo_rows(0), oo_rows(1)], axis=1).reshape(k8, nv)
        v1_ref[:, 8 * ib:8 * ib + 8, :] = dot(l1[...], w).reshape(nv, 8, nv)

    for buf, out, ssem, rsem, h, cnt, base in (
            (px, qx, p_sem.at[0], qx_sem, (1, 0, 0), NX, 0), (py, qy, p_sem.at[1], qy_sem, (0, 1, 0), NY, NX)):
        def add(ab, _, buf=buf, out=out, ssem=ssem, rsem=rsem, h=h, base=base):
            send_p(buf, out, ssem, rsem, h, ab).wait_recv()
            rows = pl.ds(pl.multiple_of((ab + base) * 8, 8), 8)
            v2_ref[:, rows, 0:128] += out[ab, 0:no]
            ext = out[ab, no:no + 8]
            v2_ref[0:8, rows, 128:176] += ext[:, :, 0:48]
            v2_ref[8:16, rows, 128:176] += pltpu.roll(ext, 80, 2)[:, :, 0:48]
            return 0
        lax.fori_loop(0, cnt, add, 0)

    wait_send(sx.at[pl.ds(0, 6)], s_sem.at[0])
    wait_send(sy.at[pl.ds(0, 6)], s_sem.at[1])
    wait_send(sp.at[pl.ds(0, nd - 1)], s_sem.at[2])
    wait_send(px, p_sem.at[0])
    wait_send(py, p_sem.at[1])


def solution(mesh):
    nd = mesh.shape["dev"]

    def local_part(a, co, cv):
        np_, n = a.shape[0], a.shape[1]
        no, nv = co.shape[1], cv.shape[1]
        npair, nb = np_ // 2, nv // 8
        ny = nb - NX
        lanes = -(-npair * nv // 128) * 128
        vm = pl.BlockSpec(memory_space=pltpu.VMEM)
        dma = pltpu.SemaphoreType.DMA
        v1, v2 = pl.pallas_call(
            functools.partial(kernel, np_, n, no, nv),
            out_shape=(jax.ShapeDtypeStruct((nv, no * no // nd, nv), F32),
                       jax.ShapeDtypeStruct((no, nv, no * nv // nd), F32)),
            in_specs=[pl.BlockSpec(memory_space=pl.ANY), vm, vm],
            out_specs=(vm, vm),
            scratch_shapes=[
                pltpu.VMEM((4, n, n, n), BF16),
                pltpu.VMEM((no * 8, n * 8), BF16),
                pltpu.VMEM((512, 512), BF16),
                pltpu.VMEM((n, nv), BF16),
                pltpu.VMEM((nd, n, 512), BF16),
                pltpu.VMEM((nd, n, 512), BF16),
                pltpu.VMEM((2, no * 8, npair * 32), BF16),
                pltpu.VMEM((2, no * 8, npair * 32), BF16),
                pltpu.VMEM((nv * 8, npair * 128), BF16),
                pltpu.VMEM((nd, npair, NX, 8, 384), BF16),
                pltpu.VMEM((nd, npair, ny, 8, 384), BF16),
                pltpu.VMEM((nd, npair, 4 * no, nv), BF16),
                pltpu.VMEM((nd, 4 * no, lanes), BF16),
                pltpu.VMEM((2, 4, npair, NX, 8, 384), BF16),
                pltpu.VMEM((2, 4, npair, ny, 8, 384), BF16),
                pltpu.VMEM((nd, 4 * no, lanes), BF16),
                pltpu.VMEM((nd, npair, 4 * no, nv), BF16),
                pltpu.VMEM((NX, no + 8, 8, 128), F32),
                pltpu.VMEM((ny, no + 8, 8, 128), F32),
                pltpu.VMEM((NX, no + 8, 8, 128), F32),
                pltpu.VMEM((ny, no + 8, 8, 128), F32),
                dma((4,)), dma((3,)), dma((2,)), dma((2,)), dma,
                dma((2,)), dma((NX,)), dma((ny,)),
            ],
            compiler_params=pltpu.CompilerParams(
                collective_id=0, has_side_effects=True, vmem_limit_bytes=44 * 1024 * 1024),
        )(a, co.T, cv.T)
        return v1.transpose(0, 2, 1), v2

    return jax.shard_map(local_part, mesh=mesh,
                         in_specs=(P(('frag', 'dev')), P('frag'), P('frag')),
                         out_specs=(P('frag', None, 'dev'), P('frag', None, 'dev')),
                         check_vma=False)
```

```python
import functools

import jax
import jax.numpy as jnp
from jax import lax
from jax.experimental import pallas as pl
from jax.experimental.pallas import tpu as pltpu
from jax.sharding import PartitionSpec as P

MESH = pl.DeviceIdType.MESH
F32 = jnp.float32
BF16 = jnp.bfloat16
NX = 6


def dot(a, b):
    return jnp.dot(a, b, preferred_element_type=F32)


def dot_t(a, b):
    return lax.dot_general(a, b, (((0,), (0,)), ((), ())), preferred_element_type=F32)


def iota(shape, d):
    return lax.broadcasted_iota(jnp.int32, shape, d)


def onehot(cond):
    return jnp.where(cond, 1.0, 0.0).astype(BF16)


def kernel(np_, n, no, nv, a_ref, cot_ref, cvt_ref, v1_ref, v2_ref,
           a_buf, la, ww, cv_buf, t_buf, h_buf, lx, ly, l1,
           sx, sy, so, sp, rx, ry, rp, ro, px, py, qx, qy,
           a_sem, s_sem, rx_sem, ry_sem, ro_sem, p_sem, qx_sem, qy_sem):
    nd = 8
    npair = np_ // 2
    nb = nv // 8
    NY = nb - NX
    ng = n // 16
    me = lax.axis_index("dev")
    frag = lax.axis_index("frag")
    y, x, c = me // 4, (me // 2) % 2, me % 2

    def dev(k):
        dy, dx, dc = k
        return (1 - y if dy else y) * 4 + (1 - x if dx else x) * 2 + (1 - c if dc else c)

    def did(k):
        return (frag, dev(k))

    KS = [(1, 1, 0), (1, 1, 1), (1, 0, 1), (0, 1, 1), (1, 0, 0), (0, 1, 0), (0, 0, 1), (0, 0, 0)]

    def a_copy(p, g):
        slot = p % 4
        return pltpu.make_async_copy(a_ref.at[p, pl.ds(16 * g, 16)], a_buf.at[slot, pl.ds(16 * g, 16)],
                                     a_sem.at[slot])

    for p in range(2):
        for g in range(ng):
            a_copy(p, g).start()

    barrier = pltpu.get_barrier_semaphore()
    for k in KS[:-1]:
        pl.semaphore_signal(barrier, inc=1, device_id=did(k), device_id_type=MESH)

    cot = cot_ref[...]
    cvt = cvt_ref[...]
    co = dot_t(cot, onehot(iota((no, no), 0) == iota((no, no), 1))).astype(BF16)
    cv = dot_t(cvt, onehot(iota((nv, nv), 0) == iota((nv, nv), 1))).astype(BF16)
    cv_buf[...] = cv
    rep8 = onehot(iota((no * 8, no), 0) // 8 == iota((no * 8, no), 1))
    tile = onehot(iota((n, 8 * n), 0) == iota((n, 8 * n), 1) % n)
    m = dot(rep8, dot(cot, tile).astype(BF16))
    la[...] = jnp.where(iota(m.shape, 0) % 8 == iota(m.shape, 1) // n, m, 0.0).astype(BF16)
    ww[...] = jnp.zeros_like(ww)
    for par in range(2):
        for j in range(2):
            jb = iota((nv, 256), 0) + j * nv
            sel_v = onehot(iota((nv, 256), 1) == jnp.where(jb < 128, jb, jb + 32 + 48 * par))
            sel_o = onehot(iota((no, 256), 1) == iota((no, 256), 0) + 128 + no * j)
            ww[par, 128 * j:128 * j + n, :] = (dot(cv, sel_v) + dot(co, sel_o)).astype(BF16)

    for p in range(2, 4):
        for g in range(ng):
            a_copy(p, g).start()

    def kron(tab, m_, kk, p_of_col, same):
        perm = onehot(iota((n, kk), 0) == p_of_col(iota((n, kk), 1)))
        r = onehot(iota((m_ * 8, m_), 0) // 8 == iota((m_ * 8, m_), 1))
        v = dot(r, dot(tab, perm).astype(BF16))
        return jnp.where(iota(v.shape, 0) % 8 == same(iota(v.shape, 1)), v, 0.0).astype(BF16)

    def send_x(i, k):
        h = (0, k[1], k[2])
        return pltpu.make_async_remote_copy(
            src_ref=sx.at[dev(k), i], dst_ref=rx.at[k[0], x * 2 + c, i],
            send_sem=s_sem.at[0], recv_sem=rx_sem.at[k[0]], device_id=did(h), device_id_type=MESH)

    def send_y(i, k):
        h = (k[0], 0, k[2])
        return pltpu.make_async_remote_copy(
            src_ref=sy.at[dev(k), i], dst_ref=ry.at[k[1], y * 2 + c, i],
            send_sem=s_sem.at[1], recv_sem=ry_sem.at[k[1]], device_id=did(h), device_id_type=MESH)

    def send_o(k):
        return pltpu.make_async_remote_copy(
            src_ref=sp.at[dev(k)], dst_ref=rp.at[me],
            send_sem=s_sem.at[2], recv_sem=ro_sem, device_id=did(k), device_id_type=MESH)

    def far_x(k):
        return bool(k[1] or k[2])

    def far_y(k):
        return bool(k[0] or k[2])

    def send_relay(i, k):
        if far_x(k) and k[0]:
            send_x(i, k).start()
        if far_y(k) and k[1]:
            send_y(i, k).start()

    def send_direct(i):
        for k in KS:
            if far_x(k) and not k[0]:
                send_x(i, k).start()
            if far_y(k) and not k[1]:
                send_y(i, k).start()

    zpad = jnp.zeros((8 * n, 128 - n), BF16)

    def pair(i, _):
        for par in range(2):
            p = 2 * i + par
            slot = p % 4

            pltpu.make_async_copy(a_ref.at[p], a_buf.at[slot], a_sem.at[slot]).wait()
            for g in range(ng):
                a0 = a_buf[slot, 16 * g:16 * g + 8].reshape(8 * n, n)
                a1 = a_buf[slot, 16 * g + 8:16 * g + 16].reshape(8 * n, n)
                w = jnp.concatenate([a0, zpad, a1, zpad], axis=1)
                t = dot(la[...], w)
                for xx in range(no):
                    tx = t[8 * xx:8 * xx + 8]
                    tx = jnp.concatenate([tx[:, 0:128], tx[:, 128:256]], axis=0).astype(BF16)
                    l0 = (xx % 2) * 128
                    t_buf[par, xx // 2, 16 * g:16 * g + 16, l0:l0 + 128] = tx

            @pl.when(p + 4 < np_)
            def _():
                for g in range(ng):
                    a_copy(p + 4, g).start()

            h_buf[par] = dot(t_buf[par].reshape(nd * n, 256), ww[par]).astype(BF16).reshape(nd, n, 256)

        for k in KS:
            d = dev(k)
            h0 = h_buf[0, d]
            h1 = h_buf[1, d]
            h = jnp.concatenate([h0[:, 0:128], h1[:, 0:128], h0[:, 128:256] + h1[:, 128:256]], axis=1)
            g = dot(cvt_ref[...], h).astype(BF16).reshape(nb, 8, 384)
            if far_x(k):
                sx[d, i] = g[0:NX]
            else:
                rx[k[0], x * 2 + c, i] = g[0:NX]
            if far_y(k):
                sy[d, i] = g[NX:nb]
            else:
                ry[k[1], y * 2 + c, i] = g[NX:nb]
            so[d, i, 0:2 * no] = dot_t(h0[:, 128:160], cv_buf[...]).astype(BF16)
            so[d, i, 2 * no:4 * no] = dot_t(h1[:, 128:160], cv_buf[...]).astype(BF16)

        @pl.when(i == 0)
        def _():
            pl.semaphore_wait(barrier, nd - 1)

        for k in KS:
            send_relay(i, k)
        send_direct(i)
        return 0

    lax.fori_loop(0, npair, pair, 0)
    def pack(d, _):
        sp[d, :, 0:npair * nv] = jnp.concatenate([so[d, i] for i in range(npair)], axis=1)
        return 0
    lax.fori_loop(0, nd, pack, 0)
    rp[me] = sp[me]
    for k in KS[:-1]:
        send_o(k).start()

    k4 = npair * 32
    for par in range(2):
        lx[par] = kron(cot, no, k4, lambda t: np_ * (y * 4 + t // (8 * npair)) + 2 * ((t // 8) % npair) + par,
                       lambda t: t % 8)
        ly[par] = kron(cot, no, k4, lambda t: np_ * (t // (16 * npair) * 4 + x * 2 + t // (8 * npair) % 2) + 2 * ((t // 8) % npair) + par,
                       lambda t: t % 8)

    def wait_recv(buf, sem):
        pltpu.make_async_remote_copy(
            src_ref=buf, dst_ref=buf, send_sem=s_sem.at[0], recv_sem=sem,
            device_id=did((0, 0, 1)), device_id_type=MESH).wait_recv()

    def wait_send(buf, sem):
        pltpu.make_async_remote_copy(
            src_ref=buf, dst_ref=buf, send_sem=sem, recv_sem=ro_sem,
            device_id=did((0, 0, 1)), device_id_type=MESH).wait_send()

    def wait_v2(w):
        wait_recv(rx.at[w, pl.ds(0, 3)], rx_sem.at[w])
        wait_recv(ry.at[w, pl.ds(0, 3)], ry_sem.at[w])

    def partial(r, left, w, ab):
        v = r[w, :, :, ab].reshape(k4, 384)
        main = dot(left[0], v[:, 0:128]) + dot(left[1], v[:, 128:256])
        even = dot(left[0], v[:, 256:384])
        odd = dot(left[1], v[:, 256:384])
        return main.reshape(no, 8, 128), even.reshape(no, 8, 128), odd.reshape(no, 8, 128)

    def send_p(buf, out, ssem, rsem, h, ab):
        return pltpu.make_async_remote_copy(
            src_ref=buf.at[ab], dst_ref=out.at[ab], send_sem=ssem, recv_sem=rsem.at[ab],
            device_id=did(h), device_id_type=MESH)

    wait_v2(1)
    for r, left, buf, out, ssem, rsem, h, cnt in (
            (rx, lx, px, qx, p_sem.at[0], qx_sem, (1, 0, 0), NX), (ry, ly, py, qy, p_sem.at[1], qy_sem, (0, 1, 0), NY)):
        def relay(ab, _, r=r, left=left, buf=buf, out=out, ssem=ssem, rsem=rsem, h=h):
            main, even, odd = partial(r, left, 1, ab)
            buf[ab, 0:no] = main
            ext = (even + pltpu.roll(odd, 80, 2))[:, :, 32:80]
            for q in range(no // 8):
                row = jnp.concatenate([ext[8 * q + t] for t in range(8)], axis=1)
                for t in range(3):
                    buf[ab, no + 3 * q + t] = row[:, 128 * t:128 * t + 128]
            send_p(buf, out, ssem, rsem, h, ab).start()
            return 0
        lax.fori_loop(0, cnt, relay, 0)

    wait_v2(0)
    for r, left, cnt, base in ((rx, lx, NX, 0), (ry, ly, NY, NX)):
        def own(ab, _, r=r, left=left, base=base):
            main, even, odd = partial(r, left, 0, ab)
            rows = pl.ds(pl.multiple_of((ab + base) * 8, 8), 8)
            v2_ref[:, rows, 0:128] = main
            v2_ref[:, rows, 128:176] = pltpu.roll(even + pltpu.roll(odd, 80, 2), 96, 2)[:, :, 0:48]
            return 0
        lax.fori_loop(0, cnt, own, 0)

    k8 = npair * 128
    l1[...] = kron(cvt_ref[...], nv, k8,
                   lambda t: np_ * (t // (16 * npair)) + 2 * ((t // 16) % npair) + (t // 8) % 2,
                   lambda t: t % 8)

    wait_recv(rp.at[pl.ds(0, nd - 1)], ro_sem)

    def unpack(d, _):
        v = rp[d]
        for i in range(npair):
            ro[d, i] = v[:, nv * i:nv * i + nv]
        return 0
    lax.fori_loop(0, nd, unpack, 0)

    for ib in range(4):
        def oo_rows(par):
            return ro[:, :, par * 32 + 8 * ib:par * 32 + 8 * ib + 8].reshape(npair * nd, 8, nv)
        w = jnp.concatenate([oo_rows(0), oo_rows(1)], axis=1).reshape(k8, nv)
        v1_ref[:, 8 * ib:8 * ib + 8, :] = dot(l1[...], w).reshape(nv, 8, nv)

    for buf, out, ssem, rsem, h, cnt, base in (
            (px, qx, p_sem.at[0], qx_sem, (1, 0, 0), NX, 0), (py, qy, p_sem.at[1], qy_sem, (0, 1, 0), NY, NX)):
        def add(ab, _, buf=buf, out=out, ssem=ssem, rsem=rsem, h=h, base=base):
            send_p(buf, out, ssem, rsem, h, ab).wait_recv()
            rows = pl.ds(pl.multiple_of((ab + base) * 8, 8), 8)
            v2_ref[:, rows, 0:128] += out[ab, 0:no]
            for q in range(no // 8):
                row = jnp.concatenate([out[ab, no + 3 * q + t] for t in range(3)], axis=1)
                for t in range(8):
                    v2_ref[8 * q + t, rows, 128:176] += row[:, 48 * t:48 * t + 48]
            return 0
        lax.fori_loop(0, cnt, add, 0)

    wait_send(sx.at[pl.ds(0, 6)], s_sem.at[0])
    wait_send(sy.at[pl.ds(0, 6)], s_sem.at[1])
    wait_send(sp.at[pl.ds(0, nd - 1)], s_sem.at[2])
    wait_send(px, p_sem.at[0])
    wait_send(py, p_sem.at[1])


def solution(mesh):
    nd = mesh.shape["dev"]

    def local_part(a, co, cv):
        np_, n = a.shape[0], a.shape[1]
        no, nv = co.shape[1], cv.shape[1]
        npair, nb = np_ // 2, nv // 8
        ny = nb - NX
        lanes = -(-npair * nv // 128) * 128
        vm = pl.BlockSpec(memory_space=pltpu.VMEM)
        dma = pltpu.SemaphoreType.DMA
        v1, v2 = pl.pallas_call(
            functools.partial(kernel, np_, n, no, nv),
            out_shape=(jax.ShapeDtypeStruct((nv, no * no // nd, nv), F32),
                       jax.ShapeDtypeStruct((no, nv, no * nv // nd), F32)),
            in_specs=[pl.BlockSpec(memory_space=pl.ANY), vm, vm],
            out_specs=(vm, vm),
            scratch_shapes=[
                pltpu.VMEM((4, n, n, n), BF16),
                pltpu.VMEM((no * 8, n * 8), BF16),
                pltpu.VMEM((2, 256, 256), BF16),
                pltpu.VMEM((n, nv), BF16),
                pltpu.VMEM((2, nd, n, 256), BF16),
                pltpu.VMEM((2, nd, n, 256), BF16),
                pltpu.VMEM((2, no * 8, npair * 32), BF16),
                pltpu.VMEM((2, no * 8, npair * 32), BF16),
                pltpu.VMEM((nv * 8, npair * 128), BF16),
                pltpu.VMEM((nd, npair, NX, 8, 384), BF16),
                pltpu.VMEM((nd, npair, ny, 8, 384), BF16),
                pltpu.VMEM((nd, npair, 4 * no, nv), BF16),
                pltpu.VMEM((nd, 4 * no, lanes), BF16),
                pltpu.VMEM((2, 4, npair, NX, 8, 384), BF16),
                pltpu.VMEM((2, 4, npair, ny, 8, 384), BF16),
                pltpu.VMEM((nd, 4 * no, lanes), BF16),
                pltpu.VMEM((nd, npair, 4 * no, nv), BF16),
                pltpu.VMEM((NX, no + 3 * no // 8, 8, 128), F32),
                pltpu.VMEM((ny, no + 3 * no // 8, 8, 128), F32),
                pltpu.VMEM((NX, no + 3 * no // 8, 8, 128), F32),
                pltpu.VMEM((ny, no + 3 * no // 8, 8, 128), F32),
                dma((4,)), dma((3,)), dma((2,)), dma((2,)), dma,
                dma((2,)), dma((NX,)), dma((ny,)),
            ],
            compiler_params=pltpu.CompilerParams(
                collective_id=0, has_side_effects=True, vmem_limit_bytes=44 * 1024 * 1024),
        )(a, co.T, cv.T)
        return v1.transpose(0, 2, 1), v2

    return jax.shard_map(local_part, mesh=mesh,
                         in_specs=(P(('frag', 'dev')), P('frag'), P('frag')),
                         out_specs=(P('frag', None, 'dev'), P('frag', None, 'dev')),
                         check_vma=False)
```

```python
import functools

import jax
import jax.numpy as jnp
from jax import lax
from jax.experimental import pallas as pl
from jax.experimental.pallas import tpu as pltpu
from jax.sharding import PartitionSpec as P

MESH = pl.DeviceIdType.MESH
F32 = jnp.float32
BF16 = jnp.bfloat16
NF = 6
EXT = 48


def dot(a, b):
    return jnp.dot(a, b, preferred_element_type=F32)


def dot_t(a, b):
    return lax.dot_general(a, b, (((0,), (0,)), ((), ())), preferred_element_type=F32)


def iota(shape, d):
    return lax.broadcasted_iota(jnp.int32, shape, d)


def onehot(cond):
    return jnp.where(cond, 1.0, 0.0).astype(BF16)


def tiles(blocks):
    return 2 * blocks + -(-2 * EXT * blocks // 128)


def kernel(np_, n, no, nv, a_ref, cot_hbm, cvt_hbm, v1_ref, v2_ref,
           cot_ref, cvt_ref, a_buf, la, ww, cv_buf, t_buf, h_buf, lf, ls, l1,
           sf, ss, so, sp, rf, rs, rp, ro, pf, ps, qf, qs,
           c_sem, a_sem, s_sem, rf_sem, rs_sem, ro_sem, p_sem, qf_sem, qs_sem):
    nd = 8
    npair = np_ // 2
    nb = nv // 8
    NS = nb - NF
    ng = n // 16
    me = lax.axis_index("dev")
    frag = lax.axis_index("frag")
    y, x, c = me // 4, (me // 2) % 2, me % 2

    def first(cd):
        return x + cd * (y - x)

    def second(cd):
        return y + cd * (x - y)

    def dev(s, f, cd, core):
        return (s + cd * (f - s)) * 4 + (f + cd * (s - f)) * 2 + core

    def flip(v, on):
        return 1 - v if on else v

    def dest(k):
        cd = flip(c, k[2])
        return dev(flip(second(cd), k[0]), flip(first(cd), k[1]), cd, cd)

    KS = [(1, 1, 0), (1, 1, 1), (1, 0, 1), (0, 1, 1), (1, 0, 0), (0, 1, 0), (0, 0, 1), (0, 0, 0)]

    def a_copy(p, g):
        slot = p % 4
        return pltpu.make_async_copy(a_ref.at[p, pl.ds(16 * g, 16)], a_buf.at[slot, pl.ds(16 * g, 16)],
                                     a_sem.at[slot])

    barrier = pltpu.get_barrier_semaphore()
    for k in KS[:-1]:
        pl.semaphore_signal(barrier, inc=1, device_id=(frag, dest(k)), device_id_type=MESH)
    coefs = [pltpu.make_async_copy(cot_hbm, cot_ref, c_sem.at[0]),
             pltpu.make_async_copy(cvt_hbm, cvt_ref, c_sem.at[1])]
    for cp in coefs:
        cp.start()
    for p in range(2):
        for g in range(ng):
            a_copy(p, g).start()
    for cp in coefs:
        cp.wait()

    cot = cot_ref[...]
    cvt = cvt_ref[...]
    co = dot_t(cot, onehot(iota((no, no), 0) == iota((no, no), 1))).astype(BF16)
    cv = dot_t(cvt, onehot(iota((nv, nv), 0) == iota((nv, nv), 1))).astype(BF16)
    cv_buf[...] = cv
    rep8 = onehot(iota((no * 8, no), 0) // 8 == iota((no * 8, no), 1))
    tile = onehot(iota((n, 8 * n), 0) == iota((n, 8 * n), 1) % n)
    m = dot(rep8, dot(cot, tile).astype(BF16))
    la[...] = jnp.where(iota(m.shape, 0) % 8 == iota(m.shape, 1) // n, m, 0.0).astype(BF16)
    ww[...] = jnp.zeros_like(ww)
    for par in range(2):
        for j in range(2):
            jb = iota((nv, 256), 0) + j * nv
            sel_v = onehot(iota((nv, 256), 1) == jnp.where(jb < 128, jb, jb + 32 + EXT * par))
            sel_o = onehot(iota((no, 256), 1) == iota((no, 256), 0) + 128 + no * j)
            ww[par, 128 * j:128 * j + n, :] = (dot(cv, sel_v) + dot(co, sel_o)).astype(BF16)

    for p in range(2, 4):
        for g in range(ng):
            a_copy(p, g).start()

    def send_f(i, k):
        cd = flip(c, k[2])
        return pltpu.make_async_remote_copy(
            src_ref=sf.at[dest(k), i], dst_ref=rf.at[k[0], first(cd) * 2 + c, i],
            send_sem=s_sem.at[0], recv_sem=rf_sem.at[k[0]],
            device_id=(frag, dev(second(cd), flip(first(cd), k[1]), cd, cd)), device_id_type=MESH)

    def send_s(i, k):
        cd = flip(c, k[2])
        return pltpu.make_async_remote_copy(
            src_ref=ss.at[dest(k), i], dst_ref=rs.at[k[1], second(cd) * 2 + c, i],
            send_sem=s_sem.at[1], recv_sem=rs_sem.at[k[1]],
            device_id=(frag, dev(flip(second(cd), k[0]), first(cd), cd, cd)), device_id_type=MESH)

    def send_o(k):
        return pltpu.make_async_remote_copy(
            src_ref=sp.at[dest(k)], dst_ref=rp.at[me],
            send_sem=s_sem.at[2], recv_sem=ro_sem, device_id=(frag, dest(k)), device_id_type=MESH)

    def far_f(k):
        return bool(k[1] or k[2])

    def far_s(k):
        return bool(k[0] or k[2])

    lane = iota((8, 128), 1)

    def put(buf, idx, g, blocks):
        for t, b in enumerate(blocks):
            for par in range(2):
                buf[idx + (2 * t + par,)] = g[8 * b:8 * b + 8, 128 * par:128 * par + 128].astype(BF16)
        rolled = []
        for t, b in enumerate(blocks):
            sh = (2 * EXT * t - 32) % 128
            rolled.append(pltpu.roll(g[8 * b:8 * b + 8, 256:384], sh, 1))
        nt = len(blocks)
        for u in range(tiles(nt) - 2 * nt):
            parts = [t for t in range(nt) if 96 * t < 128 * u + 128 and 96 * t + 96 > 128 * u]
            v = rolled[parts[0]]
            for t in parts[1:]:
                v = jnp.where(lane < 96 * t - 128 * u, v, rolled[t])
            buf[idx + (2 * nt + u,)] = v.astype(BF16)

    zpad = jnp.zeros((8 * n, 128 - n), BF16)

    def pair(i, _):
        for par in range(2):
            p = 2 * i + par
            slot = p % 4
            pltpu.make_async_copy(a_ref.at[p], a_buf.at[slot], a_sem.at[slot]).wait()
            for g in range(ng):
                a0 = a_buf[slot, 16 * g:16 * g + 8].reshape(8 * n, n)
                a1 = a_buf[slot, 16 * g + 8:16 * g + 16].reshape(8 * n, n)
                w = jnp.concatenate([a0, zpad, a1, zpad], axis=1)
                t = dot(la[...], w)
                for xx in range(no):
                    tx = t[8 * xx:8 * xx + 8]
                    tx = jnp.concatenate([tx[:, 0:128], tx[:, 128:256]], axis=0).astype(BF16)
                    l0 = (xx % 2) * 128
                    t_buf[par, xx // 2, 16 * g:16 * g + 16, l0:l0 + 128] = tx

            @pl.when(p + 4 < np_)
            def _():
                for g in range(ng):
                    a_copy(p + 4, g).start()

            h_buf[par] = dot(t_buf[par].reshape(nd * n, 256), ww[par]).astype(BF16).reshape(nd, n, 256)

        for k in KS:
            d = dest(k)
            cd = flip(c, k[2])
            h0 = h_buf[0, d]
            h1 = h_buf[1, d]
            h = jnp.concatenate([h0[:, 0:128], h1[:, 0:128], h0[:, 128:256] + h1[:, 128:256]], axis=1)
            g = dot(cvt_ref[...], h)
            if far_f(k):
                put(sf, (d, i), g, range(NF))
            else:
                put(rf, (k[0], first(cd) * 2 + c, i), g, range(NF))
            if far_s(k):
                put(ss, (d, i), g, range(NF, nb))
            else:
                put(rs, (k[1], second(cd) * 2 + c, i), g, range(NF, nb))
            so[d, i, 0:2 * no] = dot_t(h0[:, 128:160], cv_buf[...]).astype(BF16)
            so[d, i, 2 * no:4 * no] = dot_t(h1[:, 128:160], cv_buf[...]).astype(BF16)

        @pl.when(i == 0)
        def _():
            pl.semaphore_wait(barrier, nd - 1)

        for relayed in (1, 0):
            for k in KS:
                if far_f(k) and k[0] == relayed:
                    send_f(i, k).start()
                if far_s(k) and k[1] == relayed:
                    send_s(i, k).start()
        return 0

    lax.fori_loop(0, npair, pair, 0)

    def pack(d, _):
        sp[d, :, 0:npair * nv] = jnp.concatenate([so[d, i] for i in range(npair)], axis=1)
        return 0
    lax.fori_loop(0, nd, pack, 0)
    rp[me] = sp[me]
    for k in KS[:-1]:
        send_o(k).start()

    def kron(tab, m_, kk, p_of_col):
        perm = onehot(iota((n, kk), 0) == p_of_col(iota((n, kk), 1)))
        r = onehot(iota((m_ * 8, m_), 0) // 8 == iota((m_ * 8, m_), 1))
        v = dot(r, dot(tab, perm).astype(BF16))
        return jnp.where(iota(v.shape, 0) % 8 == iota(v.shape, 1) % 8, v, 0.0).astype(BF16)

    k4 = npair * 32
    for par in range(2):
        def p_f(t):
            src = t // (8 * npair)
            return np_ * dev(second(c), src // 2, c, src % 2) + 2 * ((t // 8) % npair) + par

        def p_s(t):
            src = t // (8 * npair)
            return np_ * dev(src // 2, first(c), c, src % 2) + 2 * ((t // 8) % npair) + par

        lf[par] = kron(cot_ref[...], no, k4, p_f)
        ls[par] = kron(cot_ref[...], no, k4, p_s)

    def wait_recv(buf, sem):
        pltpu.make_async_remote_copy(
            src_ref=buf, dst_ref=buf, send_sem=s_sem.at[0], recv_sem=sem,
            device_id=(frag, dest((0, 0, 1))), device_id_type=MESH).wait_recv()

    def wait_send(buf, sem):
        pltpu.make_async_remote_copy(
            src_ref=buf, dst_ref=buf, send_sem=sem, recv_sem=ro_sem,
            device_id=(frag, dest((0, 0, 1))), device_id_type=MESH).wait_send()

    lane_k = iota((k4, 128), 1)

    def partial(r, left, w, t, nt):
        def rows(u):
            return r[w, :, :, u].reshape(k4, 128)
        u, off = 96 * t // 128, 96 * t % 128
        e = rows(2 * nt + u)
        if off + 96 > 128:
            e = jnp.where(lane_k >= off, e, rows(2 * nt + u + 1))
        r0 = dot(left[0], jnp.concatenate([rows(2 * t), e], axis=1))
        r1 = dot(left[1], jnp.concatenate([rows(2 * t + 1), e], axis=1))
        main = r0[:, 0:128] + r1[:, 0:128]
        ext = r0[:, 128:256] + pltpu.roll(r1[:, 128:256], 128 - EXT, 1)
        if off:
            ext = pltpu.roll(ext, 128 - off, 1)
        return main.reshape(no, 8, 128), ext.reshape(no, 8, 128)

    def send_p(buf, out, ssem, rsem, h, t):
        return pltpu.make_async_remote_copy(
            src_ref=buf.at[t], dst_ref=out.at[t], send_sem=ssem, recv_sem=rsem.at[t],
            device_id=(frag, dest(h)), device_id_type=MESH)

    F = (rf, lf, pf, qf, p_sem.at[0], qf_sem, (1, 0, 0), NF, 0)
    S = (rs, ls, ps, qs, p_sem.at[1], qs_sem, (0, 1, 0), NS, NF)
    order = [(q, t) for t in range(NF) for q in (F, S) if t < q[7]]

    wait_recv(rf.at[1, pl.ds(0, 3)], rf_sem.at[1])
    wait_recv(rs.at[1, pl.ds(0, 3)], rs_sem.at[1])
    for (r, left, buf, out, ssem, rsem, h, nt, _), t in order:
        main, ext = partial(r, left, 1, t, nt)
        buf[t, 0:no] = main
        for q in range(no // 8):
            row = jnp.concatenate([ext[8 * q + v][:, 0:EXT] for v in range(8)], axis=1)
            for v in range(3):
                buf[t, no + 3 * q + v] = row[:, 128 * v:128 * v + 128]
        send_p(buf, out, ssem, rsem, h, t).start()

    wait_recv(rf.at[0, pl.ds(0, 3)], rf_sem.at[0])
    wait_recv(rs.at[0, pl.ds(0, 3)], rs_sem.at[0])
    for (r, left, _, _, _, _, _, nt, base), t in order:
        main, ext = partial(r, left, 0, t, nt)
        r0 = 8 * (base + t)
        v2_ref[:, r0:r0 + 8, 0:128] = main
        v2_ref[:, r0:r0 + 8, 128:128 + EXT] = ext[:, :, 0:EXT]

    k8 = npair * 128
    l1[...] = kron(cvt_ref[...], nv, k8,
                   lambda t: np_ * (t // (16 * npair)) + 2 * ((t // 16) % npair) + (t // 8) % 2)

    wait_recv(rp.at[pl.ds(0, nd - 1)], ro_sem)

    def unpack(d, _):
        v = rp[d]
        for i in range(npair):
            ro[d, i] = v[:, nv * i:nv * i + nv]
        return 0
    lax.fori_loop(0, nd, unpack, 0)

    for ib in range(4):
        def oo_rows(par):
            return ro[:, :, par * 32 + 8 * ib:par * 32 + 8 * ib + 8].reshape(npair * nd, 8, nv)
        w = jnp.concatenate([oo_rows(0), oo_rows(1)], axis=1).reshape(k8, nv)
        v1_ref[:, 8 * ib:8 * ib + 8, :] = dot(l1[...], w).reshape(nv, 8, nv)

    for (_, _, buf, out, ssem, rsem, h, nt, base), t in order:
        send_p(buf, out, ssem, rsem, h, t).wait_recv()
        r0 = 8 * (base + t)
        v2_ref[:, r0:r0 + 8, 0:128] += out[t, 0:no]
        for q in range(no // 8):
            row = jnp.concatenate([out[t, no + 3 * q + v] for v in range(3)], axis=1)
            for v in range(8):
                v2_ref[8 * q + v, r0:r0 + 8, 128:128 + EXT] += row[:, EXT * v:EXT * v + EXT]

    wait_send(sf.at[pl.ds(0, 6)], s_sem.at[0])
    wait_send(ss.at[pl.ds(0, 6)], s_sem.at[1])
    wait_send(sp.at[pl.ds(0, nd - 1)], s_sem.at[2])
    wait_send(pf, p_sem.at[0])
    wait_send(ps, p_sem.at[1])


def solution(mesh):
    nd = mesh.shape["dev"]

    def local_part(a, co, cv):
        np_, n = a.shape[0], a.shape[1]
        no, nv = co.shape[1], cv.shape[1]
        npair, nb = np_ // 2, nv // 8
        ns = nb - NF
        lanes = -(-npair * nv // 128) * 128
        vm = pl.BlockSpec(memory_space=pltpu.VMEM)
        hbm = pl.BlockSpec(memory_space=pltpu.HBM)
        dma = pltpu.SemaphoreType.DMA
        v1, v2 = pl.pallas_call(
            functools.partial(kernel, np_, n, no, nv),
            out_shape=(jax.ShapeDtypeStruct((nv, no * no // nd, nv), F32),
                       jax.ShapeDtypeStruct((no, nv, no * nv // nd), F32)),
            in_specs=[hbm, hbm, hbm],
            out_specs=(vm, vm),
            scratch_shapes=[
                pltpu.VMEM((no, n), BF16),
                pltpu.VMEM((nv, n), BF16),
                pltpu.VMEM((4, n, n, n), BF16),
                pltpu.VMEM((no * 8, n * 8), BF16),
                pltpu.VMEM((2, 256, 256), BF16),
                pltpu.VMEM((n, nv), BF16),
                pltpu.VMEM((2, nd, n, 256), BF16),
                pltpu.VMEM((2, nd, n, 256), BF16),
                pltpu.VMEM((2, no * 8, npair * 32), BF16),
                pltpu.VMEM((2, no * 8, npair * 32), BF16),
                pltpu.VMEM((nv * 8, npair * 128), BF16),
                pltpu.VMEM((nd, npair, tiles(NF), 8, 128), BF16),
                pltpu.VMEM((nd, npair, tiles(ns), 8, 128), BF16),
                pltpu.VMEM((nd, npair, 4 * no, nv), BF16),
                pltpu.VMEM((nd, 4 * no, lanes), BF16),
                pltpu.VMEM((2, 4, npair, tiles(NF), 8, 128), BF16),
                pltpu.VMEM((2, 4, npair, tiles(ns), 8, 128), BF16),
                pltpu.VMEM((nd, 4 * no, lanes), BF16),
                pltpu.VMEM((nd, npair, 4 * no, nv), BF16),
                pltpu.VMEM((NF, no + 3 * no // 8, 8, 128), F32),
                pltpu.VMEM((ns, no + 3 * no // 8, 8, 128), F32),
                pltpu.VMEM((NF, no + 3 * no // 8, 8, 128), F32),
                pltpu.VMEM((ns, no + 3 * no // 8, 8, 128), F32),
                dma((2,)), dma((4,)), dma((3,)), dma((2,)), dma((2,)), dma,
                dma((2,)), dma((NF,)), dma((ns,)),
            ],
            compiler_params=pltpu.CompilerParams(
                collective_id=0, has_side_effects=True, vmem_limit_bytes=44 * 1024 * 1024),
        )(a, co.T, cv.T)
        return v1.transpose(0, 2, 1), v2

    return jax.shard_map(local_part, mesh=mesh,
                         in_specs=(P(('frag', 'dev')), P('frag'), P('frag')),
                         out_specs=(P('frag', None, 'dev'), P('frag', None, 'dev')),
                         check_vma=False)
```

```python
import functools

import jax
import jax.numpy as jnp
from jax import lax
from jax.experimental import pallas as pl
from jax.experimental.pallas import tpu as pltpu
from jax.sharding import PartitionSpec as P

MESH = pl.DeviceIdType.MESH
F32 = jnp.float32
BF16 = jnp.bfloat16
NF = 6
EXT = 48


def dot(a, b):
    return jnp.dot(a, b, preferred_element_type=F32)


def dot_t(a, b):
    return lax.dot_general(a, b, (((0,), (0,)), ((), ())), preferred_element_type=F32)


def iota(shape, d):
    return lax.broadcasted_iota(jnp.int32, shape, d)


def onehot(cond):
    return jnp.where(cond, 1.0, 0.0).astype(BF16)


def tiles(blocks):
    return 2 * blocks + -(-2 * EXT * blocks // 128)


def kernel(np_, n, no, nv, a_ref, cot_hbm, cvt_hbm, v1_ref, v2_ref,
           cot_ref, cvt_ref, a_buf, la, ww, cvs, t_buf, h_buf, lf, ls, l1,
           sf, ss, sp, rf, rs, rp, ro, pf, ps, qf, qs,
           c_sem, a_sem, s_sem, rf_sem, rs_sem, ro_sem, p_sem, qf_sem, qs_sem, d_sem):
    nd = 8
    npair = np_ // 2
    nb = nv // 8
    NS = nb - NF
    ng = n // 16
    me = lax.axis_index("dev")
    frag = lax.axis_index("frag")
    y, x, c = me // 4, (me // 2) % 2, me % 2

    def first(cd):
        return x + cd * (y - x)

    def second(cd):
        return y + cd * (x - y)

    def dev(s, f, cd, core):
        return (s + cd * (f - s)) * 4 + (f + cd * (s - f)) * 2 + core

    def flip(v, on):
        return 1 - v if on else v

    def dest(k):
        cd = flip(c, k[2])
        return dev(flip(second(cd), k[0]), flip(first(cd), k[1]), cd, cd)

    KS = [(1, 1, 0), (1, 1, 1), (1, 0, 1), (0, 1, 1), (1, 0, 0), (0, 1, 0), (0, 0, 1), (0, 0, 0)]
    NEAR = [k for k in KS[:-1] if not (k[0] and k[1])]

    def a_copy(p, g):
        slot = p % 4
        return pltpu.make_async_copy(a_ref.at[p, pl.ds(16 * g, 16)], a_buf.at[slot, pl.ds(16 * g, 16)],
                                     a_sem.at[slot])

    barrier = pltpu.get_barrier_semaphore()
    for k in NEAR:
        pl.semaphore_signal(barrier, inc=1, device_id=(frag, dest(k)), device_id_type=MESH)
    coefs = [pltpu.make_async_copy(cot_hbm, cot_ref, c_sem.at[0]),
             pltpu.make_async_copy(cvt_hbm, cvt_ref, c_sem.at[1])]
    for cp in coefs:
        cp.start()
    for g in range(ng):
        a_copy(0, g).start()
    for cp in coefs:
        cp.wait()

    cot = cot_ref[...]
    cvt = cvt_ref[...]
    co = dot_t(cot, onehot(iota((no, no), 0) == iota((no, no), 1))).astype(BF16)
    cv = dot_t(cvt, onehot(iota((nv, nv), 0) == iota((nv, nv), 1))).astype(BF16)
    rep8 = onehot(iota((no * 8, no), 0) // 8 == iota((no * 8, no), 1))
    tile = onehot(iota((n, 8 * n), 0) == iota((n, 8 * n), 1) % n)
    m = dot(rep8, dot(cot, tile).astype(BF16))
    la[...] = jnp.where(iota(m.shape, 0) % 8 == iota(m.shape, 1) // n, m, 0.0).astype(BF16)
    for g in range(ng):
        a_copy(1, g).start()
    ww[...] = jnp.zeros_like(ww)
    for par in range(2):
        for j in range(2):
            jb = iota((nv, 256), 0) + j * nv
            sel_v = onehot(iota((nv, 256), 1) == jnp.where(jb < 128, jb, jb + 32 + EXT * par))
            sel_o = onehot(iota((no, 256), 1) == iota((no, 256), 0) + 128 + 32 * par + no * j)
            ww[par, 128 * j:128 * j + n, :] = (dot(cv, sel_v) + dot(co, sel_o)).astype(BF16)

    for p in range(2, 4):
        for g in range(ng):
            a_copy(p, g).start()

    def span(part, nt):
        return {None: pl.ds(0, tiles(nt)), 0: pl.ds(0, nt), 1: pl.ds(nt, tiles(nt) - nt)}[part]

    def send_f(i, k, part=None):
        cd = flip(c, k[2])
        part = span(part, NF)
        return pltpu.make_async_remote_copy(
            src_ref=sf.at[dest(k), i, part], dst_ref=rf.at[k[0], first(cd) * 2 + c, i, part],
            send_sem=s_sem.at[0], recv_sem=rf_sem.at[k[0]],
            device_id=(frag, dev(second(cd), flip(first(cd), k[1]), cd, cd)), device_id_type=MESH)

    def send_s(i, k, part=None):
        cd = flip(c, k[2])
        part = span(part, NS)
        return pltpu.make_async_remote_copy(
            src_ref=ss.at[dest(k), i, part], dst_ref=rs.at[k[1], second(cd) * 2 + c, i, part],
            send_sem=s_sem.at[1], recv_sem=rs_sem.at[k[1]],
            device_id=(frag, dev(flip(second(cd), k[0]), first(cd), cd, cd)), device_id_type=MESH)

    def send_o(k):
        return pltpu.make_async_remote_copy(
            src_ref=sp.at[dest(k), pl.ds(0, rp.shape[1])], dst_ref=rp.at[me],
            send_sem=s_sem.at[2], recv_sem=ro_sem, device_id=(frag, dest(k)), device_id_type=MESH)

    def far_f(k):
        return bool(k[1] or k[2])

    def far_s(k):
        return bool(k[0] or k[2])

    lane = iota((8, 128), 1)

    def put_row(buf, idx, par, g, blocks):
        for t, b in enumerate(blocks):
            buf[idx + (len(blocks) * par + t,)] = g[8 * b:8 * b + 8].astype(BF16)

    def put_ext(buf, idx, g, blocks):
        rolled = []
        for t, b in enumerate(blocks):
            rolled.append(pltpu.roll(g[8 * b:8 * b + 8], (2 * EXT * t - 32) % 128, 1))
        nt = len(blocks)
        for u in range(tiles(nt) - 2 * nt):
            parts = [t for t in range(nt) if 96 * t < 128 * u + 128 and 96 * t + 96 > 128 * u]
            v = rolled[parts[0]]
            for t in parts[1:]:
                v = jnp.where(lane < 96 * t - 128 * u, v, rolled[t])
            buf[idx + (2 * nt + u,)] = v.astype(BF16)

    def places(i, k):
        d = dest(k)
        cd = flip(c, k[2])
        return ((sf, (d, i), range(NF)) if far_f(k) else (rf, (k[0], first(cd) * 2 + c, i), range(NF)),
                (ss, (d, i), range(NF, nb)) if far_s(k) else (rs, (k[1], second(cd) * 2 + c, i), range(NF, nb)))

    zpad = jnp.zeros((8 * n, 128 - n), BF16)
    lane_n = iota((n, 128), 1)

    def wait_row(p):
        pltpu.make_async_copy(a_ref.at[p], a_buf.at[p % 4], a_sem.at[p % 4]).wait()

    def steps12(p, par):
        slot = p % 4
        for g in range(ng):
            a0 = a_buf[slot, 16 * g:16 * g + 8].reshape(8 * n, n)
            a1 = a_buf[slot, 16 * g + 8:16 * g + 16].reshape(8 * n, n)
            w = jnp.concatenate([a0, zpad, a1, zpad], axis=1)
            t = dot(la[...], w)
            for xx in range(no):
                tx = t[8 * xx:8 * xx + 8]
                tx = jnp.concatenate([tx[:, 0:128], tx[:, 128:256]], axis=0).astype(BF16)
                l0 = (xx % 2) * 128
                t_buf[par, xx // 2, 16 * g:16 * g + 16, l0:l0 + 128] = tx
        for e in range(0, nd, 4):
            hh = dot(t_buf[par, e:e + 4].reshape(4 * n, 256), ww[par])
            h_buf[par, e:e + 4] = hh.astype(BF16).reshape(4, n, 256)

    def step3(i, rows):
        for k in KS:
            d = dest(k)
            hs = [h_buf[0, d], h_buf[1, d]]
            e0, e1 = hs[0][:, 128:256], hs[1][:, 128:256]
            cols = [hs[par][:, 0:128] for par in rows]
            if 1 in rows:
                cols.append(jnp.where(lane_n < 80, e0, e1))
            g = dot(cvt_ref[...], jnp.concatenate(cols, axis=1) if len(cols) > 1 else cols[0])
            for buf, idx, blocks in places(i, k):
                for q, par in enumerate(rows):
                    put_row(buf, idx, par, g[:, 128 * q:128 * q + 128], blocks)
                if 1 in rows:
                    put_ext(buf, idx, g[:, 128 * len(rows):], blocks)
            if 1 in rows:
                go = dot_t(jnp.where(lane_n < 32, e0, e1)[:, 0:64], cvs[i]).astype(BF16)
                for u in range(2):
                    sp[d, nv * i // 128 + u] += go[:, 128 * u:128 * u + 128]

    def sends(i, part=None):
        for relayed in (1, 0):
            for k in KS:
                if far_f(k) and k[0] == relayed:
                    send_f(i, k, part).start()
                if far_s(k) and k[1] == relayed:
                    send_s(i, k, part).start()

    def pair(i, _):
        wait_row(2 * i)
        wait_row(2 * i + 1)
        steps12(2 * i, 0)
        steps12(2 * i + 1, 1)
        step3(i, (0, 1))

        @pl.when(2 * i + 4 < np_)
        def _():
            for p in (2 * i + 4, 2 * i + 5):
                for g in range(ng):
                    a_copy(p, g).start()

        sends(i)
        return 0

    wait_row(0)
    steps12(0, 0)
    step3(0, (0,))
    pl.semaphore_wait(barrier, len(NEAR))
    sends(0, 0)
    pl.semaphore_signal(d_sem, inc=1, device_id=(frag, dest((0, 1, 0))), device_id_type=MESH)
    sp[...] = jnp.zeros_like(sp)
    for i in range(npair):
        cvs[i] = dot(cv, onehot(iota((nv, 256), 1) == iota((nv, 256), 0) + nv * i % 128)).astype(BF16)
    wait_row(1)
    steps12(1, 1)
    step3(0, (1,))
    for p in (4, 5):
        for g in range(ng):
            a_copy(p, g).start()
    sends(0, 1)

    lax.fori_loop(1, npair, pair, 0)

    pl.semaphore_wait(d_sem, 1)
    nt = rp.shape[1]
    rp[me] = sp[me, 0:nt]
    for k in KS[:-1]:
        send_o(k).start()

    def kron(tab, m_, kk, p_of_col):
        perm = onehot(iota((n, kk), 0) == p_of_col(iota((n, kk), 1)))
        r = onehot(iota((m_ * 8, m_), 0) // 8 == iota((m_ * 8, m_), 1))
        v = dot(r, dot(tab, perm).astype(BF16))
        return jnp.where(iota(v.shape, 0) % 8 == iota(v.shape, 1) % 8, v, 0.0).astype(BF16)

    k4 = npair * 32
    for par in range(2):
        def p_f(t):
            src = t // (8 * npair)
            return np_ * dev(second(c), src // 2, c, src % 2) + 2 * ((t // 8) % npair) + par

        def p_s(t):
            src = t // (8 * npair)
            return np_ * dev(src // 2, first(c), c, src % 2) + 2 * ((t // 8) % npair) + par

        lf[par] = kron(cot_ref[...], no, k4, p_f)
        ls[par] = kron(cot_ref[...], no, k4, p_s)

    def wait_recv(buf, sem):
        pltpu.make_async_remote_copy(
            src_ref=buf, dst_ref=buf, send_sem=s_sem.at[0], recv_sem=sem,
            device_id=(frag, dest((0, 0, 1))), device_id_type=MESH).wait_recv()

    def wait_send(buf, sem):
        pltpu.make_async_remote_copy(
            src_ref=buf, dst_ref=buf, send_sem=sem, recv_sem=ro_sem,
            device_id=(frag, dest((0, 0, 1))), device_id_type=MESH).wait_send()

    lane_k = iota((k4, 128), 1)

    def partial(r, left, w, t, nt):
        def rows(u):
            return r[w, :, :, u].reshape(k4, 128)
        u, off = 96 * t // 128, 96 * t % 128
        e = rows(2 * nt + u)
        if off + 96 > 128:
            e = jnp.where(lane_k >= off, e, rows(2 * nt + u + 1))
        r0 = dot(left[0], jnp.concatenate([rows(t), e], axis=1))
        r1 = dot(left[1], jnp.concatenate([rows(nt + t), e], axis=1))
        main = r0[:, 0:128] + r1[:, 0:128]
        ext = r0[:, 128:256] + pltpu.roll(r1[:, 128:256], 128 - EXT, 1)
        if off:
            ext = pltpu.roll(ext, 128 - off, 1)
        return main.reshape(no, 8, 128), ext.reshape(no, 8, 128)

    def send_p(buf, out, ssem, rsem, h, t):
        return pltpu.make_async_remote_copy(
            src_ref=buf.at[t], dst_ref=out.at[t], send_sem=ssem, recv_sem=rsem.at[t],
            device_id=(frag, dest(h)), device_id_type=MESH)

    F = (rf, lf, pf, qf, p_sem.at[0], qf_sem, (1, 0, 0), NF, 0)
    S = (rs, ls, ps, qs, p_sem.at[1], qs_sem, (0, 1, 0), NS, NF)
    order = [(q, t) for t in range(NF) for q in (F, S) if t < q[7]]

    wait_recv(rf.at[1, pl.ds(0, 3)], rf_sem.at[1])
    wait_recv(rs.at[1, pl.ds(0, 3)], rs_sem.at[1])
    for (r, left, buf, out, ssem, rsem, h, nt, _), t in order:
        main, ext = partial(r, left, 1, t, nt)
        buf[t, 0:no] = main
        for q in range(no // 8):
            row = jnp.concatenate([ext[8 * q + v][:, 0:EXT] for v in range(8)], axis=1)
            for v in range(3):
                buf[t, no + 3 * q + v] = row[:, 128 * v:128 * v + 128]
        send_p(buf, out, ssem, rsem, h, t).start()

    wait_recv(rf.at[0, pl.ds(0, 3)], rf_sem.at[0])
    wait_recv(rs.at[0, pl.ds(0, 3)], rs_sem.at[0])
    for (r, left, _, _, _, _, _, nt, base), t in order:
        main, ext = partial(r, left, 0, t, nt)
        r0 = 8 * (base + t)
        v2_ref[:, r0:r0 + 8, 0:128] = main
        v2_ref[:, r0:r0 + 8, 128:128 + EXT] = ext[:, :, 0:EXT]

    k8 = npair * 128
    l1[...] = kron(cvt_ref[...], nv, k8,
                   lambda t: np_ * (t // (16 * npair)) + 2 * ((t // 16) % npair) + (t // 8) % 2)

    wait_recv(rp.at[pl.ds(0, nd - 1)], ro_sem)

    def unpack(d, _):
        v = jnp.concatenate([rp[d, u] for u in range(rp.shape[1])], axis=1)
        for i in range(npair):
            ro[d, i] = v[:, nv * i:nv * i + nv]
        return 0
    lax.fori_loop(0, nd, unpack, 0)

    for ib in range(4):
        def oo_rows(par):
            return ro[:, :, par * 32 + 8 * ib:par * 32 + 8 * ib + 8].reshape(npair * nd, 8, nv)
        w = jnp.concatenate([oo_rows(0), oo_rows(1)], axis=1).reshape(k8, nv)
        v1_ref[:, 8 * ib:8 * ib + 8, :] = dot(l1[...], w).reshape(nv, 8, nv)

    for (_, _, buf, out, ssem, rsem, h, nt, base), t in order:
        send_p(buf, out, ssem, rsem, h, t).wait_recv()
        r0 = 8 * (base + t)
        v2_ref[:, r0:r0 + 8, 0:128] += out[t, 0:no]
        for q in range(no // 8):
            row = jnp.concatenate([out[t, no + 3 * q + v] for v in range(3)], axis=1)
            for v in range(8):
                v2_ref[8 * q + v, r0:r0 + 8, 128:128 + EXT] += row[:, EXT * v:EXT * v + EXT]

    wait_send(sf.at[pl.ds(0, 6)], s_sem.at[0])
    wait_send(ss.at[pl.ds(0, 6)], s_sem.at[1])
    wait_send(rp.at[pl.ds(0, nd - 1)], s_sem.at[2])
    wait_send(pf, p_sem.at[0])
    wait_send(ps, p_sem.at[1])


def solution(mesh):
    nd = mesh.shape["dev"]

    def local_part(a, co, cv):
        np_, n = a.shape[0], a.shape[1]
        no, nv = co.shape[1], cv.shape[1]
        npair, nb = np_ // 2, nv // 8
        ns = nb - NF
        lanes = -(-npair * nv // 128)
        vm = pl.BlockSpec(memory_space=pltpu.VMEM)
        hbm = pl.BlockSpec(memory_space=pltpu.HBM)
        dma = pltpu.SemaphoreType.DMA
        v1, v2 = pl.pallas_call(
            functools.partial(kernel, np_, n, no, nv),
            out_shape=(jax.ShapeDtypeStruct((nv, no * no // nd, nv), F32),
                       jax.ShapeDtypeStruct((no, nv, no * nv // nd), F32)),
            in_specs=[hbm, hbm, hbm],
            out_specs=(vm, vm),
            scratch_shapes=[
                pltpu.VMEM((no, n), BF16),
                pltpu.VMEM((nv, n), BF16),
                pltpu.VMEM((4, n, n, n), BF16),
                pltpu.VMEM((no * 8, n * 8), BF16),
                pltpu.VMEM((2, 256, 256), BF16),
                pltpu.VMEM((npair, n, 256), BF16),
                pltpu.VMEM((2, nd, n, 256), BF16),
                pltpu.VMEM((2, nd, n, 256), BF16),
                pltpu.VMEM((2, no * 8, npair * 32), BF16),
                pltpu.VMEM((2, no * 8, npair * 32), BF16),
                pltpu.VMEM((nv * 8, npair * 128), BF16),
                pltpu.VMEM((nd, npair, tiles(NF), 8, 128), BF16),
                pltpu.VMEM((nd, npair, tiles(ns), 8, 128), BF16),
                pltpu.VMEM((nd, lanes + 1, 4 * no, 128), BF16),
                pltpu.VMEM((2, 4, npair, tiles(NF), 8, 128), BF16),
                pltpu.VMEM((2, 4, npair, tiles(ns), 8, 128), BF16),
                pltpu.VMEM((nd, lanes, 4 * no, 128), BF16),
                pltpu.VMEM((nd, npair, 4 * no, nv), BF16),
                pltpu.VMEM((NF, no + 3 * no // 8, 8, 128), F32),
                pltpu.VMEM((ns, no + 3 * no // 8, 8, 128), F32),
                pltpu.VMEM((NF, no + 3 * no // 8, 8, 128), F32),
                pltpu.VMEM((ns, no + 3 * no // 8, 8, 128), F32),
                dma((2,)), dma((4,)), dma((3,)), dma((2,)), dma((2,)), dma,
                dma((2,)), dma((NF,)), dma((ns,)), pltpu.SemaphoreType.REGULAR,
            ],
            compiler_params=pltpu.CompilerParams(
                collective_id=0, has_side_effects=True, vmem_limit_bytes=44 * 1024 * 1024),
        )(a, *(pltpu.with_memory_space_constraint(t.T, pltpu.HBM) for t in (co, cv)))
        return v1.transpose(0, 2, 1), v2

    return jax.shard_map(local_part, mesh=mesh,
                         in_specs=(P(('frag', 'dev')), P('frag'), P('frag')),
                         out_specs=(P('frag', None, 'dev'), P('frag', None, 'dev')),
                         check_vma=False)
```

```python
import functools

import jax
import jax.numpy as jnp
from jax import lax
from jax.experimental import pallas as pl
from jax.experimental.pallas import tpu as pltpu
from jax.sharding import PartitionSpec as P

MESH = pl.DeviceIdType.MESH
F32 = jnp.float32
BF16 = jnp.bfloat16
NF = 6
SLOTS = 6
EXT = 48


def dot(a, b):
    return jnp.dot(a, b, preferred_element_type=F32)


def dot_t(a, b):
    return lax.dot_general(a, b, (((0,), (0,)), ((), ())), preferred_element_type=F32)


def iota(shape, d):
    return lax.broadcasted_iota(jnp.int32, shape, d)


def onehot(cond):
    return jnp.where(cond, 1.0, 0.0).astype(BF16)


def tiles(blocks):
    return 2 * blocks + -(-2 * EXT * blocks // 128)


def kernel(np_, n, no, nv, a_ref, cot_hbm, cvt_hbm, v1_ref, v2_ref,
           cot_ref, cvt_ref, a_buf, la, ww, cvs, t_buf, h_buf, lf, ls, l1,
           sf, ss, sp, rf, rs, rp, ro, pf, ps, qf, qs,
           c_sem, a_sem, s_sem, rf_sem, rs_sem, ro_sem, p_sem, qf_sem, qs_sem, d_sem):
    nd = 8
    npair = np_ // 2
    nb = nv // 8
    NS = nb - NF
    ng = n // 16
    me = lax.axis_index("dev")
    frag = lax.axis_index("frag")
    y, x, c = me // 4, (me // 2) % 2, me % 2

    def first(cd):
        return x + cd * (y - x)

    def second(cd):
        return y + cd * (x - y)

    def dev(s, f, cd, core):
        return (s + cd * (f - s)) * 4 + (f + cd * (s - f)) * 2 + core

    def flip(v, on):
        return 1 - v if on else v

    def dest(k):
        cd = flip(c, k[2])
        return dev(flip(second(cd), k[0]), flip(first(cd), k[1]), cd, cd)

    KS = [(1, 1, 0), (1, 1, 1), (1, 0, 1), (0, 1, 1), (1, 0, 0), (0, 1, 0), (0, 0, 1), (0, 0, 0)]
    NEAR = [k for k in KS[:-1] if not (k[0] and k[1])]

    def row_copy(p):
        return pltpu.make_async_copy(a_ref.at[p], a_buf.at[p % SLOTS], a_sem.at[p % SLOTS])

    barrier = pltpu.get_barrier_semaphore()
    for k in NEAR:
        pl.semaphore_signal(barrier, inc=1, device_id=(frag, dest(k)), device_id_type=MESH)
    coefs = [pltpu.make_async_copy(cot_hbm, cot_ref, c_sem.at[0]),
             pltpu.make_async_copy(cvt_hbm, cvt_ref, c_sem.at[1])]
    for cp in coefs:
        cp.start()
    row_copy(0).start()
    for cp in coefs:
        cp.wait()

    cot = cot_ref[...]
    cvt = cvt_ref[...]
    co = dot_t(cot, onehot(iota((no, no), 0) == iota((no, no), 1))).astype(BF16)
    cv = dot_t(cvt, onehot(iota((nv, nv), 0) == iota((nv, nv), 1))).astype(BF16)
    rep8 = onehot(iota((no * 8, no), 0) // 8 == iota((no * 8, no), 1))
    tile = onehot(iota((n, 8 * n), 0) == iota((n, 8 * n), 1) % n)
    m = dot(rep8, dot(cot, tile).astype(BF16))
    la[...] = jnp.where(iota(m.shape, 0) % 8 == iota(m.shape, 1) // n, m, 0.0).astype(BF16)
    row_copy(1).start()
    ww[...] = jnp.zeros_like(ww)
    for par in range(2):
        for j in range(2):
            jb = iota((nv, 256), 0) + j * nv
            sel_v = onehot(iota((nv, 256), 1) == jnp.where(jb < 128, jb, jb + 32 + EXT * par))
            sel_o = onehot(iota((no, 256), 1) == iota((no, 256), 0) + 128 + 32 * par + no * j)
            ww[par, 128 * j:128 * j + n, :] = (dot(cv, sel_v) + dot(co, sel_o)).astype(BF16)

    for p in range(2, SLOTS):
        row_copy(p).start()

    def span(part, nt):
        return {None: pl.ds(0, tiles(nt)), 0: pl.ds(0, nt), 1: pl.ds(nt, tiles(nt) - nt)}[part]

    def send_f(i, k, part=None):
        cd = flip(c, k[2])
        part = span(part, NF)
        return pltpu.make_async_remote_copy(
            src_ref=sf.at[dest(k), i, part], dst_ref=rf.at[k[0], first(cd) * 2 + c, i, part],
            send_sem=s_sem.at[0], recv_sem=rf_sem.at[k[0]],
            device_id=(frag, dev(second(cd), flip(first(cd), k[1]), cd, cd)), device_id_type=MESH)

    def send_s(i, k, part=None):
        cd = flip(c, k[2])
        part = span(part, NS)
        return pltpu.make_async_remote_copy(
            src_ref=ss.at[dest(k), i, part], dst_ref=rs.at[k[1], second(cd) * 2 + c, i, part],
            send_sem=s_sem.at[1], recv_sem=rs_sem.at[k[1]],
            device_id=(frag, dev(flip(second(cd), k[0]), first(cd), cd, cd)), device_id_type=MESH)

    def send_o(k):
        return pltpu.make_async_remote_copy(
            src_ref=sp.at[dest(k), pl.ds(0, rp.shape[1])], dst_ref=rp.at[me],
            send_sem=s_sem.at[2], recv_sem=ro_sem, device_id=(frag, dest(k)), device_id_type=MESH)

    def far_f(k):
        return bool(k[1] or k[2])

    def far_s(k):
        return bool(k[0] or k[2])

    lane = iota((8, 128), 1)

    def put_row(buf, idx, par, g, blocks):
        for t, b in enumerate(blocks):
            buf[idx + (len(blocks) * par + t,)] = g[8 * b:8 * b + 8].astype(BF16)

    def put_ext(buf, idx, g, blocks):
        rolled = []
        for t, b in enumerate(blocks):
            rolled.append(pltpu.roll(g[8 * b:8 * b + 8], (2 * EXT * t - 32) % 128, 1))
        nt = len(blocks)
        for u in range(tiles(nt) - 2 * nt):
            parts = [t for t in range(nt) if 96 * t < 128 * u + 128 and 96 * t + 96 > 128 * u]
            v = rolled[parts[0]]
            for t in parts[1:]:
                v = jnp.where(lane < 96 * t - 128 * u, v, rolled[t])
            buf[idx + (2 * nt + u,)] = v.astype(BF16)

    def places(i, k):
        d = dest(k)
        cd = flip(c, k[2])
        return ((sf, (d, i), range(NF)) if far_f(k) else (rf, (k[0], first(cd) * 2 + c, i), range(NF)),
                (ss, (d, i), range(NF, nb)) if far_s(k) else (rs, (k[1], second(cd) * 2 + c, i), range(NF, nb)))

    zpad = jnp.zeros((8 * n, 128 - n), BF16)
    lane_n = iota((n, 128), 1)

    def wait_row(p):
        row_copy(p).wait()

    def steps12(p, par):
        slot = p % SLOTS
        for g in range(ng):
            a0 = a_buf[slot, 16 * g:16 * g + 8].reshape(8 * n, n)
            a1 = a_buf[slot, 16 * g + 8:16 * g + 16].reshape(8 * n, n)
            w = jnp.concatenate([a0, zpad, a1, zpad], axis=1)
            t = dot(la[...], w)
            for xx in range(no):
                tx = t[8 * xx:8 * xx + 8]
                tx = jnp.concatenate([tx[:, 0:128], tx[:, 128:256]], axis=0).astype(BF16)
                l0 = (xx % 2) * 128
                t_buf[par, xx // 2, 16 * g:16 * g + 16, l0:l0 + 128] = tx
        for e in range(0, nd, 4):
            hh = dot(t_buf[par, e:e + 4].reshape(4 * n, 256), ww[par])
            h_buf[par, e:e + 4] = hh.astype(BF16).reshape(4, n, 256)

    def step3(i, rows):
        for k in KS:
            d = dest(k)
            hs = [h_buf[0, d], h_buf[1, d]]
            e0, e1 = hs[0][:, 128:256], hs[1][:, 128:256]
            cols = [hs[par][:, 0:128] for par in rows]
            if 1 in rows:
                cols.append(jnp.where(lane_n < 80, e0, e1))
            g = dot(cvt_ref[...], jnp.concatenate(cols, axis=1) if len(cols) > 1 else cols[0])
            for buf, idx, blocks in places(i, k):
                for q, par in enumerate(rows):
                    put_row(buf, idx, par, g[:, 128 * q:128 * q + 128], blocks)
                if 1 in rows:
                    put_ext(buf, idx, g[:, 128 * len(rows):], blocks)
            if 1 in rows:
                go = dot_t(jnp.where(lane_n < 32, e0, e1)[:, 0:64], cvs[i]).astype(BF16)
                for u in range(2):
                    sp[d, nv * i // 128 + u] += go[:, 128 * u:128 * u + 128]

    def sends(i, part=None):
        for relayed in (1, 0):
            for k in KS:
                if far_f(k) and k[0] == relayed:
                    send_f(i, k, part).start()
                if far_s(k) and k[1] == relayed:
                    send_s(i, k, part).start()

    def pair(i, _):
        wait_row(2 * i)
        wait_row(2 * i + 1)
        steps12(2 * i, 0)
        steps12(2 * i + 1, 1)
        step3(i, (0, 1))

        sends(i)

        @pl.when(2 * i + SLOTS < np_)
        def _():
            for p in (2 * i + SLOTS, 2 * i + SLOTS + 1):
                row_copy(p).start()

        return 0

    wait_row(0)
    steps12(0, 0)
    step3(0, (0,))
    pl.semaphore_wait(barrier, len(NEAR))
    sends(0, 0)
    pl.semaphore_signal(d_sem, inc=1, device_id=(frag, dest((0, 1, 0))), device_id_type=MESH)
    sp[...] = jnp.zeros_like(sp)
    for i in range(npair):
        cvs[i] = dot(cv, onehot(iota((nv, 256), 1) == iota((nv, 256), 0) + nv * i % 128)).astype(BF16)
    wait_row(1)
    steps12(1, 1)
    step3(0, (1,))
    sends(0, 1)
    for p in (SLOTS, SLOTS + 1):
        row_copy(p).start()

    lax.fori_loop(1, npair, pair, 0)

    pl.semaphore_wait(d_sem, 1)
    nt = rp.shape[1]
    rp[me] = sp[me, 0:nt]
    for k in KS[:-1]:
        send_o(k).start()

    def kron(tab, m_, kk, p_of_col):
        perm = onehot(iota((n, kk), 0) == p_of_col(iota((n, kk), 1)))
        r = onehot(iota((m_ * 8, m_), 0) // 8 == iota((m_ * 8, m_), 1))
        v = dot(r, dot(tab, perm).astype(BF16))
        return jnp.where(iota(v.shape, 0) % 8 == iota(v.shape, 1) % 8, v, 0.0).astype(BF16)

    k4 = npair * 32
    for par in range(2):
        def p_f(t):
            src = t // (8 * npair)
            return np_ * dev(second(c), src // 2, c, src % 2) + 2 * ((t // 8) % npair) + par

        def p_s(t):
            src = t // (8 * npair)
            return np_ * dev(src // 2, first(c), c, src % 2) + 2 * ((t // 8) % npair) + par

        lf[par] = kron(cot_ref[...], no, k4, p_f)
        ls[par] = kron(cot_ref[...], no, k4, p_s)

    def wait_recv(buf, sem):
        pltpu.make_async_remote_copy(
            src_ref=buf, dst_ref=buf, send_sem=s_sem.at[0], recv_sem=sem,
            device_id=(frag, dest((0, 0, 1))), device_id_type=MESH).wait_recv()

    def wait_send(buf, sem):
        pltpu.make_async_remote_copy(
            src_ref=buf, dst_ref=buf, send_sem=sem, recv_sem=ro_sem,
            device_id=(frag, dest((0, 0, 1))), device_id_type=MESH).wait_send()

    lane_k = iota((k4, 128), 1)

    def partial(r, left, w, t, nt):
        def rows(u):
            return r[w, :, :, u].reshape(k4, 128)
        u, off = 96 * t // 128, 96 * t % 128
        e = rows(2 * nt + u)
        if off + 96 > 128:
            e = jnp.where(lane_k >= off, e, rows(2 * nt + u + 1))
        r0 = dot(left[0], jnp.concatenate([rows(t), e], axis=1))
        r1 = dot(left[1], jnp.concatenate([rows(nt + t), e], axis=1))
        main = r0[:, 0:128] + r1[:, 0:128]
        ext = r0[:, 128:256] + pltpu.roll(r1[:, 128:256], 128 - EXT, 1)
        if off:
            ext = pltpu.roll(ext, 128 - off, 1)
        return main.reshape(no, 8, 128), ext.reshape(no, 8, 128)

    def send_p(buf, out, ssem, rsem, h, t):
        return pltpu.make_async_remote_copy(
            src_ref=buf.at[t], dst_ref=out.at[t], send_sem=ssem, recv_sem=rsem.at[t],
            device_id=(frag, dest(h)), device_id_type=MESH)

    F = (rf, lf, pf, qf, p_sem.at[0], qf_sem, (1, 0, 0), NF, 0)
    S = (rs, ls, ps, qs, p_sem.at[1], qs_sem, (0, 1, 0), NS, NF)
    order = [(q, t) for t in range(NF) for q in (F, S) if t < q[7]]

    wait_recv(rf.at[1, pl.ds(0, 3)], rf_sem.at[1])
    wait_recv(rs.at[1, pl.ds(0, 3)], rs_sem.at[1])
    for (r, left, buf, out, ssem, rsem, h, nt, _), t in order:
        main, ext = partial(r, left, 1, t, nt)
        buf[t, 0:no] = main
        for q in range(no // 8):
            row = jnp.concatenate([ext[8 * q + v][:, 0:EXT] for v in range(8)], axis=1)
            for v in range(3):
                buf[t, no + 3 * q + v] = row[:, 128 * v:128 * v + 128]
        send_p(buf, out, ssem, rsem, h, t).start()

    wait_recv(rf.at[0, pl.ds(0, 3)], rf_sem.at[0])
    wait_recv(rs.at[0, pl.ds(0, 3)], rs_sem.at[0])
    for (r, left, _, _, _, _, _, nt, base), t in order:
        main, ext = partial(r, left, 0, t, nt)
        r0 = 8 * (base + t)
        v2_ref[:, r0:r0 + 8, 0:128] = main
        v2_ref[:, r0:r0 + 8, 128:128 + EXT] = ext[:, :, 0:EXT]

    k8 = npair * 128
    l1[...] = kron(cvt_ref[...], nv, k8,
                   lambda t: np_ * (t // (16 * npair)) + 2 * ((t // 16) % npair) + (t // 8) % 2)

    wait_recv(rp.at[pl.ds(0, nd - 1)], ro_sem)

    def unpack(d, _):
        v = jnp.concatenate([rp[d, u] for u in range(rp.shape[1])], axis=1)
        for i in range(npair):
            ro[d, i] = v[:, nv * i:nv * i + nv]
        return 0
    lax.fori_loop(0, nd, unpack, 0)

    for ib in range(4):
        def oo_rows(par):
            return ro[:, :, par * 32 + 8 * ib:par * 32 + 8 * ib + 8].reshape(npair * nd, 8, nv)
        w = jnp.concatenate([oo_rows(0), oo_rows(1)], axis=1).reshape(k8, nv)
        v1_ref[:, 8 * ib:8 * ib + 8, :] = dot(l1[...], w).reshape(nv, 8, nv)

    for (_, _, buf, out, ssem, rsem, h, nt, base), t in order:
        send_p(buf, out, ssem, rsem, h, t).wait_recv()
        r0 = 8 * (base + t)
        v2_ref[:, r0:r0 + 8, 0:128] += out[t, 0:no]
        for q in range(no // 8):
            row = jnp.concatenate([out[t, no + 3 * q + v] for v in range(3)], axis=1)
            for v in range(8):
                v2_ref[8 * q + v, r0:r0 + 8, 128:128 + EXT] += row[:, EXT * v:EXT * v + EXT]

    wait_send(sf.at[pl.ds(0, 6)], s_sem.at[0])
    wait_send(ss.at[pl.ds(0, 6)], s_sem.at[1])
    wait_send(rp.at[pl.ds(0, nd - 1)], s_sem.at[2])
    wait_send(pf, p_sem.at[0])
    wait_send(ps, p_sem.at[1])


def out_kernel(v1_ref, v2_ref, o1_ref, o2_ref, sem):
    cps = []
    for j, (v, o) in enumerate(((v1_ref, o1_ref), (v2_ref, o2_ref))):
        m = v.shape[0] // 4
        for q in range(4):
            cps.append(pltpu.make_async_copy(v.at[pl.ds(m * q, m)], o.at[pl.ds(m * q, m)], sem.at[4 * j + q]))
    for cp in cps:
        cp.start()
    for cp in cps:
        cp.wait()


def solution(mesh):
    nd = mesh.shape["dev"]

    def local_part(a, co, cv):
        np_, n = a.shape[0], a.shape[1]
        no, nv = co.shape[1], cv.shape[1]
        npair, nb = np_ // 2, nv // 8
        ns = nb - NF
        lanes = -(-npair * nv // 128)
        vm = pl.BlockSpec(memory_space=pltpu.VMEM)
        hbm = pl.BlockSpec(memory_space=pltpu.HBM)
        dma = pltpu.SemaphoreType.DMA
        v1, v2 = pl.pallas_call(
            functools.partial(kernel, np_, n, no, nv),
            out_shape=(jax.ShapeDtypeStruct((nv, no * no // nd, nv), F32),
                       jax.ShapeDtypeStruct((no, nv, no * nv // nd), F32)),
            in_specs=[hbm, hbm, hbm],
            out_specs=(vm, vm),
            scratch_shapes=[
                pltpu.VMEM((no, n), BF16),
                pltpu.VMEM((nv, n), BF16),
                pltpu.VMEM((SLOTS, n, n, n), BF16),
                pltpu.VMEM((no * 8, n * 8), BF16),
                pltpu.VMEM((2, 256, 256), BF16),
                pltpu.VMEM((npair, n, 256), BF16),
                pltpu.VMEM((2, nd, n, 256), BF16),
                pltpu.VMEM((2, nd, n, 256), BF16),
                pltpu.VMEM((2, no * 8, npair * 32), BF16),
                pltpu.VMEM((2, no * 8, npair * 32), BF16),
                pltpu.VMEM((nv * 8, npair * 128), BF16),
                pltpu.VMEM((nd, npair, tiles(NF), 8, 128), BF16),
                pltpu.VMEM((nd, npair, tiles(ns), 8, 128), BF16),
                pltpu.VMEM((nd, lanes + 1, 4 * no, 128), BF16),
                pltpu.VMEM((2, 4, npair, tiles(NF), 8, 128), BF16),
                pltpu.VMEM((2, 4, npair, tiles(ns), 8, 128), BF16),
                pltpu.VMEM((nd, lanes, 4 * no, 128), BF16),
                pltpu.VMEM((nd, npair, 4 * no, nv), BF16),
                pltpu.VMEM((NF, no + 3 * no // 8, 8, 128), F32),
                pltpu.VMEM((ns, no + 3 * no // 8, 8, 128), F32),
                pltpu.VMEM((NF, no + 3 * no // 8, 8, 128), F32),
                pltpu.VMEM((ns, no + 3 * no // 8, 8, 128), F32),
                dma((2,)), dma((SLOTS,)), dma((3,)), dma((2,)), dma((2,)), dma,
                dma((2,)), dma((NF,)), dma((ns,)), pltpu.SemaphoreType.REGULAR,
            ],
            compiler_params=pltpu.CompilerParams(
                collective_id=0, has_side_effects=True, vmem_limit_bytes=50 * 1024 * 1024),
        )(a, *(pltpu.with_memory_space_constraint(t.T, pltpu.HBM) for t in (co, cv)))
        hb = pl.BlockSpec(memory_space=pl.ANY)
        v1, v2 = pl.pallas_call(
            out_kernel,
            out_shape=(jax.ShapeDtypeStruct(v1.shape, F32), jax.ShapeDtypeStruct(v2.shape, F32)),
            in_specs=[vm, vm], out_specs=(hb, hb),
            scratch_shapes=[dma((8,))],
            compiler_params=pltpu.CompilerParams(vmem_limit_bytes=4 * 1024 * 1024),
        )(v1, v2)
        return v1.transpose(0, 2, 1), v2

    return jax.shard_map(local_part, mesh=mesh,
                         in_specs=(P(('frag', 'dev')), P('frag'), P('frag')),
                         out_specs=(P('frag', None, 'dev'), P('frag', None, 'dev')),
                         check_vma=False)
```

```python
import functools

import jax
import jax.numpy as jnp
from jax import lax
from jax.experimental import pallas as pl
from jax.experimental.pallas import tpu as pltpu
from jax.sharding import PartitionSpec as P

MESH = pl.DeviceIdType.MESH
F32 = jnp.float32
BF16 = jnp.bfloat16
NF = 6
SLOTS = 6
EXT = 48


def dot(a, b):
    return jnp.dot(a, b, preferred_element_type=F32)


def dot_t(a, b):
    return lax.dot_general(a, b, (((0,), (0,)), ((), ())), preferred_element_type=F32)


def iota(shape, d):
    return lax.broadcasted_iota(jnp.int32, shape, d)


def onehot(cond):
    return jnp.where(cond, 1.0, 0.0).astype(BF16)


def tiles(blocks):
    return 2 * blocks + -(-2 * EXT * blocks // 128)


def kernel(np_, n, no, nv, a_ref, cot_hbm, cvt_hbm, v1_ref, v2_ref,
           cot_ref, cvt_ref, a_buf, la, ww, cvs, t_buf, h_buf, lf, ls, l1,
           sf, ss, sp, rf, rs, rp, ro, pf, ps, qf, qs,
           c_sem, a_sem, s_sem, rf_sem, rs_sem, ro_sem, p_sem, qf_sem, qs_sem, d_sem):
    nd = 8
    npair = np_ // 2
    nb = nv // 8
    NS = nb - NF
    ng = n // 16
    me = lax.axis_index("dev")
    frag = lax.axis_index("frag")
    y, x, c = me // 4, (me // 2) % 2, me % 2

    def first(cd):
        return x + cd * (y - x)

    def second(cd):
        return y + cd * (x - y)

    def dev(s, f, cd, core):
        return (s + cd * (f - s)) * 4 + (f + cd * (s - f)) * 2 + core

    def flip(v, on):
        return 1 - v if on else v

    def dest(k):
        cd = flip(c, k[2])
        return dev(flip(second(cd), k[0]), flip(first(cd), k[1]), cd, cd)

    KS = [(1, 1, 0), (1, 1, 1), (1, 0, 1), (0, 1, 1), (1, 0, 0), (0, 1, 0), (0, 0, 1), (0, 0, 0)]
    NEAR = [k for k in KS[:-1] if not (k[0] and k[1])]

    def row_copy(p):
        return pltpu.make_async_copy(a_ref.at[p], a_buf.at[p % SLOTS], a_sem.at[p % SLOTS])

    barrier = pltpu.get_barrier_semaphore()
    for k in NEAR:
        pl.semaphore_signal(barrier, inc=1, device_id=(frag, dest(k)), device_id_type=MESH)
    coefs = [pltpu.make_async_copy(cot_hbm, cot_ref, c_sem.at[0]),
             pltpu.make_async_copy(cvt_hbm, cvt_ref, c_sem.at[1])]
    for cp in coefs:
        cp.start()
    row_copy(0).start()
    for cp in coefs:
        cp.wait()

    cot = cot_ref[...]
    cvt = cvt_ref[...]
    co = dot_t(cot, onehot(iota((no, no), 0) == iota((no, no), 1))).astype(BF16)
    cv = dot_t(cvt, onehot(iota((nv, nv), 0) == iota((nv, nv), 1))).astype(BF16)
    rep8 = onehot(iota((no * 8, no), 0) // 8 == iota((no * 8, no), 1))
    tile = onehot(iota((n, 8 * n), 0) == iota((n, 8 * n), 1) % n)
    m = dot(rep8, dot(cot, tile).astype(BF16))
    la[...] = jnp.where(iota(m.shape, 0) % 8 == iota(m.shape, 1) // n, m, 0.0).astype(BF16)
    row_copy(1).start()
    ww[...] = jnp.zeros_like(ww)
    for par in range(2):
        for j in range(2):
            jb = iota((nv, 256), 0) + j * nv
            sel_v = onehot(iota((nv, 256), 1) == jnp.where(jb < 128, jb, jb + 32 + EXT * par))
            sel_o = onehot(iota((no, 256), 1) == iota((no, 256), 0) + 128 + 32 * par + no * j)
            ww[par, 128 * j:128 * j + n, :] = (dot(cv, sel_v) + dot(co, sel_o)).astype(BF16)

    for p in range(2, SLOTS):
        row_copy(p).start()

    def span(part, nt):
        return {None: pl.ds(0, tiles(nt)), 0: pl.ds(0, nt), 1: pl.ds(nt, tiles(nt) - nt)}[part]

    def send_f(i, k, part=None):
        cd = flip(c, k[2])
        part = span(part, NF)
        return pltpu.make_async_remote_copy(
            src_ref=sf.at[dest(k), i, part], dst_ref=rf.at[k[0], first(cd) * 2 + c, i, part],
            send_sem=s_sem.at[0], recv_sem=rf_sem.at[k[0]],
            device_id=(frag, dev(second(cd), flip(first(cd), k[1]), cd, cd)), device_id_type=MESH)

    def send_s(i, k, part=None):
        cd = flip(c, k[2])
        part = span(part, NS)
        return pltpu.make_async_remote_copy(
            src_ref=ss.at[dest(k), i, part], dst_ref=rs.at[k[1], second(cd) * 2 + c, i, part],
            send_sem=s_sem.at[1], recv_sem=rs_sem.at[k[1]],
            device_id=(frag, dev(flip(second(cd), k[0]), first(cd), cd, cd)), device_id_type=MESH)

    def send_o(k):
        return pltpu.make_async_remote_copy(
            src_ref=sp.at[dest(k), pl.ds(0, rp.shape[1])], dst_ref=rp.at[me],
            send_sem=s_sem.at[2], recv_sem=ro_sem, device_id=(frag, dest(k)), device_id_type=MESH)

    def far_f(k):
        return bool(k[1] or k[2])

    def far_s(k):
        return bool(k[0] or k[2])

    lane = iota((8, 128), 1)

    def put_row(buf, idx, par, g, blocks):
        for t, b in enumerate(blocks):
            buf[idx + (len(blocks) * par + t,)] = g[8 * b:8 * b + 8].astype(BF16)

    def put_ext(buf, idx, g, blocks):
        rolled = []
        for t, b in enumerate(blocks):
            rolled.append(pltpu.roll(g[8 * b:8 * b + 8], (2 * EXT * t - 32) % 128, 1))
        nt = len(blocks)
        for u in range(tiles(nt) - 2 * nt):
            parts = [t for t in range(nt) if 96 * t < 128 * u + 128 and 96 * t + 96 > 128 * u]
            v = rolled[parts[0]]
            for t in parts[1:]:
                v = jnp.where(lane < 96 * t - 128 * u, v, rolled[t])
            buf[idx + (2 * nt + u,)] = v.astype(BF16)

    def places(i, k):
        d = dest(k)
        cd = flip(c, k[2])
        return ((sf, (d, i), range(NF)) if far_f(k) else (rf, (k[0], first(cd) * 2 + c, i), range(NF)),
                (ss, (d, i), range(NF, nb)) if far_s(k) else (rs, (k[1], second(cd) * 2 + c, i), range(NF, nb)))

    zpad = jnp.zeros((8 * n, 128 - n), BF16)
    lane_n = iota((n, 128), 1)

    def wait_row(p):
        row_copy(p).wait()

    def steps12(p, par):
        slot = p % SLOTS
        for g in range(ng):
            a0 = a_buf[slot, 16 * g:16 * g + 8].reshape(8 * n, n)
            a1 = a_buf[slot, 16 * g + 8:16 * g + 16].reshape(8 * n, n)
            w = jnp.concatenate([a0, zpad, a1, zpad], axis=1)
            t = dot(la[...], w)
            for xx in range(no):
                tx = t[8 * xx:8 * xx + 8]
                tx = jnp.concatenate([tx[:, 0:128], tx[:, 128:256]], axis=0).astype(BF16)
                l0 = (xx % 2) * 128
                t_buf[par, xx // 2, 16 * g:16 * g + 16, l0:l0 + 128] = tx
        for e in range(0, nd, 4):
            hh = dot(t_buf[par, e:e + 4].reshape(4 * n, 256), ww[par])
            h_buf[par, e:e + 4] = hh.astype(BF16).reshape(4, n, 256)

    def step3(i, rows):
        for k in KS:
            d = dest(k)
            hs = [h_buf[0, d], h_buf[1, d]]
            e0, e1 = hs[0][:, 128:256], hs[1][:, 128:256]
            cols = [hs[par][:, 0:128] for par in rows]
            if 1 in rows:
                cols.append(jnp.where(lane_n < 80, e0, e1))
            g = dot(cvt_ref[...], jnp.concatenate(cols, axis=1) if len(cols) > 1 else cols[0])
            for buf, idx, blocks in places(i, k):
                for q, par in enumerate(rows):
                    put_row(buf, idx, par, g[:, 128 * q:128 * q + 128], blocks)
                if 1 in rows:
                    put_ext(buf, idx, g[:, 128 * len(rows):], blocks)
            if 1 in rows:
                go = dot_t(jnp.where(lane_n < 32, e0, e1)[:, 0:64], cvs[i]).astype(BF16)
                for u in range(2):
                    sp[d, nv * i // 128 + u] += go[:, 128 * u:128 * u + 128]

    def sends(i, part=None):
        for relayed in (1, 0):
            for k in KS:
                if far_f(k) and k[0] == relayed:
                    send_f(i, k, part).start()
                if far_s(k) and k[1] == relayed:
                    send_s(i, k, part).start()

    def pair(i, _):
        wait_row(2 * i)
        wait_row(2 * i + 1)
        steps12(2 * i, 0)
        steps12(2 * i + 1, 1)
        step3(i, (0, 1))

        sends(i)

        @pl.when(2 * i + SLOTS < np_)
        def _():
            for p in (2 * i + SLOTS, 2 * i + SLOTS + 1):
                row_copy(p).start()

        return 0

    sp[...] = jnp.zeros_like(sp)
    for i in range(npair):
        cvs[i] = dot(cv, onehot(iota((nv, 256), 1) == iota((nv, 256), 0) + nv * i % 128)).astype(BF16)
    wait_row(0)
    steps12(0, 0)
    step3(0, (0,))
    pl.semaphore_wait(barrier, len(NEAR))
    sends(0, 0)
    pl.semaphore_signal(d_sem, inc=1, device_id=(frag, dest((0, 1, 0))), device_id_type=MESH)
    wait_row(1)
    steps12(1, 1)
    step3(0, (1,))
    sends(0, 1)
    for p in (SLOTS, SLOTS + 1):
        row_copy(p).start()

    wait_row(2)
    steps12(2, 0)
    step3(1, (0,))
    sends(1, 0)
    wait_row(3)
    steps12(3, 1)
    step3(1, (1,))
    sends(1, 1)
    for p in (SLOTS + 2, SLOTS + 3):
        row_copy(p).start()

    lax.fori_loop(2, npair, pair, 0)

    pl.semaphore_wait(d_sem, 1)
    nt = rp.shape[1]
    rp[me] = sp[me, 0:nt]
    for k in KS[:-1]:
        send_o(k).start()

    def kron(tab, m_, kk, p_of_col):
        perm = onehot(iota((n, kk), 0) == p_of_col(iota((n, kk), 1)))
        r = onehot(iota((m_ * 8, m_), 0) // 8 == iota((m_ * 8, m_), 1))
        v = dot(r, dot(tab, perm).astype(BF16))
        return jnp.where(iota(v.shape, 0) % 8 == iota(v.shape, 1) % 8, v, 0.0).astype(BF16)

    k4 = npair * 32
    for par in range(2):
        def p_f(t):
            src = t // (8 * npair)
            return np_ * dev(second(c), src // 2, c, src % 2) + 2 * ((t // 8) % npair) + par

        def p_s(t):
            src = t // (8 * npair)
            return np_ * dev(src // 2, first(c), c, src % 2) + 2 * ((t // 8) % npair) + par

        lf[par] = kron(cot_ref[...], no, k4, p_f)
        ls[par] = kron(cot_ref[...], no, k4, p_s)

    def wait_recv(buf, sem):
        pltpu.make_async_remote_copy(
            src_ref=buf, dst_ref=buf, send_sem=s_sem.at[0], recv_sem=sem,
            device_id=(frag, dest((0, 0, 1))), device_id_type=MESH).wait_recv()

    def wait_send(buf, sem):
        pltpu.make_async_remote_copy(
            src_ref=buf, dst_ref=buf, send_sem=sem, recv_sem=ro_sem,
            device_id=(frag, dest((0, 0, 1))), device_id_type=MESH).wait_send()

    lane_k = iota((k4, 128), 1)

    def partial(r, left, w, t, nt):
        def rows(u):
            return r[w, :, :, u].reshape(k4, 128)
        u, off = 96 * t // 128, 96 * t % 128
        e = rows(2 * nt + u)
        if off + 96 > 128:
            e = jnp.where(lane_k >= off, e, rows(2 * nt + u + 1))
        r0 = dot(left[0], jnp.concatenate([rows(t), e], axis=1))
        r1 = dot(left[1], jnp.concatenate([rows(nt + t), e], axis=1))
        main = r0[:, 0:128] + r1[:, 0:128]
        ext = r0[:, 128:256] + pltpu.roll(r1[:, 128:256], 128 - EXT, 1)
        if off:
            ext = pltpu.roll(ext, 128 - off, 1)
        return main.reshape(no, 8, 128), ext.reshape(no, 8, 128)

    def send_p(buf, out, ssem, rsem, h, t):
        return pltpu.make_async_remote_copy(
            src_ref=buf.at[t], dst_ref=out.at[t], send_sem=ssem, recv_sem=rsem.at[t],
            device_id=(frag, dest(h)), device_id_type=MESH)

    F = (rf, lf, pf, qf, p_sem.at[0], qf_sem, (1, 0, 0), NF, 0)
    S = (rs, ls, ps, qs, p_sem.at[1], qs_sem, (0, 1, 0), NS, NF)
    order = [(q, t) for t in range(NF) for q in (F, S) if t < q[7]]

    wait_recv(rf.at[1, pl.ds(0, 3)], rf_sem.at[1])
    wait_recv(rs.at[1, pl.ds(0, 3)], rs_sem.at[1])
    for (r, left, buf, out, ssem, rsem, h, nt, _), t in order:
        main, ext = partial(r, left, 1, t, nt)
        buf[t, 0:no] = main
        for q in range(no // 8):
            row = jnp.concatenate([ext[8 * q + v][:, 0:EXT] for v in range(8)], axis=1)
            for v in range(3):
                buf[t, no + 3 * q + v] = row[:, 128 * v:128 * v + 128]
        send_p(buf, out, ssem, rsem, h, t).start()

    wait_recv(rf.at[0, pl.ds(0, 3)], rf_sem.at[0])
    wait_recv(rs.at[0, pl.ds(0, 3)], rs_sem.at[0])
    for (r, left, _, _, _, _, _, nt, base), t in order:
        main, ext = partial(r, left, 0, t, nt)
        r0 = 8 * (base + t)
        v2_ref[:, r0:r0 + 8, 0:128] = main
        v2_ref[:, r0:r0 + 8, 128:128 + EXT] = ext[:, :, 0:EXT]

    k8 = npair * 128
    l1[...] = kron(cvt_ref[...], nv, k8,
                   lambda t: np_ * (t // (16 * npair)) + 2 * ((t // 16) % npair) + (t // 8) % 2)

    wait_recv(rp.at[pl.ds(0, nd - 1)], ro_sem)

    def unpack(d, _):
        v = jnp.concatenate([rp[d, u] for u in range(rp.shape[1])], axis=1)
        for i in range(npair):
            ro[d, i] = v[:, nv * i:nv * i + nv]
        return 0
    lax.fori_loop(0, nd, unpack, 0)

    for ib in range(4):
        def oo_rows(par):
            return ro[:, :, par * 32 + 8 * ib:par * 32 + 8 * ib + 8].reshape(npair * nd, 8, nv)
        w = jnp.concatenate([oo_rows(0), oo_rows(1)], axis=1).reshape(k8, nv)
        v1_ref[:, 8 * ib:8 * ib + 8, :] = dot(l1[...], w).reshape(nv, 8, nv)

    for (_, _, buf, out, ssem, rsem, h, nt, base), t in order:
        send_p(buf, out, ssem, rsem, h, t).wait_recv()
        r0 = 8 * (base + t)
        v2_ref[:, r0:r0 + 8, 0:128] += out[t, 0:no]
        for q in range(no // 8):
            row = jnp.concatenate([out[t, no + 3 * q + v] for v in range(3)], axis=1)
            for v in range(8):
                v2_ref[8 * q + v, r0:r0 + 8, 128:128 + EXT] += row[:, EXT * v:EXT * v + EXT]

    wait_send(sf.at[pl.ds(0, 6)], s_sem.at[0])
    wait_send(ss.at[pl.ds(0, 6)], s_sem.at[1])
    wait_send(rp.at[pl.ds(0, nd - 1)], s_sem.at[2])
    wait_send(pf, p_sem.at[0])
    wait_send(ps, p_sem.at[1])


def out_kernel(v1_ref, v2_ref, o1_ref, o2_ref, sem):
    cps = []
    for j, (v, o) in enumerate(((v1_ref, o1_ref), (v2_ref, o2_ref))):
        m = v.shape[0] // 4
        for q in range(4):
            cps.append(pltpu.make_async_copy(v.at[pl.ds(m * q, m)], o.at[pl.ds(m * q, m)], sem.at[4 * j + q]))
    for cp in cps:
        cp.start()
    for cp in cps:
        cp.wait()


def solution(mesh):
    nd = mesh.shape["dev"]

    def local_part(a, co, cv):
        np_, n = a.shape[0], a.shape[1]
        no, nv = co.shape[1], cv.shape[1]
        npair, nb = np_ // 2, nv // 8
        ns = nb - NF
        lanes = -(-npair * nv // 128)
        vm = pl.BlockSpec(memory_space=pltpu.VMEM)
        hbm = pl.BlockSpec(memory_space=pltpu.HBM)
        dma = pltpu.SemaphoreType.DMA
        v1, v2 = pl.pallas_call(
            functools.partial(kernel, np_, n, no, nv),
            out_shape=(jax.ShapeDtypeStruct((nv, no * no // nd, nv), F32),
                       jax.ShapeDtypeStruct((no, nv, no * nv // nd), F32)),
            in_specs=[hbm, hbm, hbm],
            out_specs=(vm, vm),
            scratch_shapes=[
                pltpu.VMEM((no, n), BF16),
                pltpu.VMEM((nv, n), BF16),
                pltpu.VMEM((SLOTS, n, n, n), BF16),
                pltpu.VMEM((no * 8, n * 8), BF16),
                pltpu.VMEM((2, 256, 256), BF16),
                pltpu.VMEM((npair, n, 256), BF16),
                pltpu.VMEM((2, nd, n, 256), BF16),
                pltpu.VMEM((2, nd, n, 256), BF16),
                pltpu.VMEM((2, no * 8, npair * 32), BF16),
                pltpu.VMEM((2, no * 8, npair * 32), BF16),
                pltpu.VMEM((nv * 8, npair * 128), BF16),
                pltpu.VMEM((nd, npair, tiles(NF), 8, 128), BF16),
                pltpu.VMEM((nd, npair, tiles(ns), 8, 128), BF16),
                pltpu.VMEM((nd, lanes + 1, 4 * no, 128), BF16),
                pltpu.VMEM((2, 4, npair, tiles(NF), 8, 128), BF16),
                pltpu.VMEM((2, 4, npair, tiles(ns), 8, 128), BF16),
                pltpu.VMEM((nd, lanes, 4 * no, 128), BF16),
                pltpu.VMEM((nd, npair, 4 * no, nv), BF16),
                pltpu.VMEM((NF, no + 3 * no // 8, 8, 128), F32),
                pltpu.VMEM((ns, no + 3 * no // 8, 8, 128), F32),
                pltpu.VMEM((NF, no + 3 * no // 8, 8, 128), F32),
                pltpu.VMEM((ns, no + 3 * no // 8, 8, 128), F32),
                dma((2,)), dma((SLOTS,)), dma((3,)), dma((2,)), dma((2,)), dma,
                dma((2,)), dma((NF,)), dma((ns,)), pltpu.SemaphoreType.REGULAR,
            ],
            compiler_params=pltpu.CompilerParams(
                collective_id=0, has_side_effects=True, vmem_limit_bytes=50 * 1024 * 1024),
        )(a, *(pltpu.with_memory_space_constraint(t.T, pltpu.HBM) for t in (co, cv)))
        hb = pl.BlockSpec(memory_space=pl.ANY)
        v1, v2 = pl.pallas_call(
            out_kernel,
            out_shape=(jax.ShapeDtypeStruct(v1.shape, F32), jax.ShapeDtypeStruct(v2.shape, F32)),
            in_specs=[vm, vm], out_specs=(hb, hb),
            scratch_shapes=[dma((8,))],
            compiler_params=pltpu.CompilerParams(vmem_limit_bytes=4 * 1024 * 1024),
        )(v1, v2)
        return v1.transpose(0, 2, 1), v2

    return jax.shard_map(local_part, mesh=mesh,
                         in_specs=(P(('frag', 'dev')), P('frag'), P('frag')),
                         out_specs=(P('frag', None, 'dev'), P('frag', None, 'dev')),
                         check_vma=False)
```

```python
import functools

import jax
import jax.numpy as jnp
from jax import lax
from jax.experimental import pallas as pl
from jax.experimental.pallas import tpu as pltpu
from jax.sharding import PartitionSpec as P

MESH = pl.DeviceIdType.MESH
F32 = jnp.float32
BF16 = jnp.bfloat16
NF = 6
SLOTS = 6
EXT = 48


def dot(a, b):
    return jnp.dot(a, b, preferred_element_type=F32)


def dot_t(a, b):
    return lax.dot_general(a, b, (((0,), (0,)), ((), ())), preferred_element_type=F32)


def iota(shape, d):
    return lax.broadcasted_iota(jnp.int32, shape, d)


def onehot(cond):
    return jnp.where(cond, 1.0, 0.0).astype(BF16)


def tiles(blocks):
    return 2 * blocks + -(-2 * EXT * blocks // 128)


def kernel(np_, n, no, nv, a_ref, cot_hbm, cvt_hbm, v1_ref, v2_ref,
           cot_ref, cvt_ref, a_buf, la, ww, cvs, t_buf, h_buf, lf, ls, l1,
           sf, ss, sp, rf, rs, rp, ro, pf, ps, qf, qs,
           c_sem, a_sem, s_sem, rf_sem, rs_sem, ro_sem, p_sem, qf_sem, qs_sem, d_sem):
    nd = 8
    npair = np_ // 2
    nb = nv // 8
    NS = nb - NF
    ng = n // 16
    me = lax.axis_index("dev")
    frag = lax.axis_index("frag")
    y, x, c = me // 4, (me // 2) % 2, me % 2

    def first(cd):
        return x + cd * (y - x)

    def second(cd):
        return y + cd * (x - y)

    def dev(s, f, cd, core):
        return (s + cd * (f - s)) * 4 + (f + cd * (s - f)) * 2 + core

    def flip(v, on):
        return 1 - v if on else v

    def dest(k):
        cd = flip(c, k[2])
        return dev(flip(second(cd), k[0]), flip(first(cd), k[1]), cd, cd)

    KS = [(1, 1, 0), (1, 1, 1), (1, 0, 1), (0, 1, 1), (1, 0, 0), (0, 1, 0), (0, 0, 1), (0, 0, 0)]
    NEAR = [k for k in KS[:-1] if not (k[0] and k[1])]

    def row_copy(p):
        return pltpu.make_async_copy(a_ref.at[p], a_buf.at[p % SLOTS], a_sem.at[p % SLOTS])

    barrier = pltpu.get_barrier_semaphore()
    for k in NEAR:
        pl.semaphore_signal(barrier, inc=1, device_id=(frag, dest(k)), device_id_type=MESH)
    coefs = [pltpu.make_async_copy(cot_hbm, cot_ref, c_sem.at[0]),
             pltpu.make_async_copy(cvt_hbm, cvt_ref, c_sem.at[1])]
    for cp in coefs:
        cp.start()
    row_copy(0).start()
    for cp in coefs:
        cp.wait()

    cot = cot_ref[...]
    cvt = cvt_ref[...]
    co = dot_t(cot, onehot(iota((no, no), 0) == iota((no, no), 1))).astype(BF16)
    cv = dot_t(cvt, onehot(iota((nv, nv), 0) == iota((nv, nv), 1))).astype(BF16)
    rep8 = onehot(iota((no * 8, no), 0) // 8 == iota((no * 8, no), 1))
    tile = onehot(iota((n, 8 * n), 0) == iota((n, 8 * n), 1) % n)
    m = dot(rep8, dot(cot, tile).astype(BF16))
    la[...] = jnp.where(iota(m.shape, 0) % 8 == iota(m.shape, 1) // n, m, 0.0).astype(BF16)
    row_copy(1).start()
    ww[...] = jnp.zeros_like(ww)
    for par in range(2):
        for j in range(2):
            jb = iota((nv, 256), 0) + j * nv
            sel_v = onehot(iota((nv, 256), 1) == jnp.where(jb < 128, jb, jb + 32 + EXT * par))
            sel_o = onehot(iota((no, 256), 1) == iota((no, 256), 0) + 128 + 32 * par + no * j)
            ww[par, 128 * j:128 * j + n, :] = (dot(cv, sel_v) + dot(co, sel_o)).astype(BF16)

    for p in range(2, SLOTS):
        row_copy(p).start()

    def span(part, nt):
        return {None: pl.ds(0, tiles(nt)), 0: pl.ds(0, nt), 1: pl.ds(nt, tiles(nt) - nt)}[part]

    def send_f(i, k, part=None):
        cd = flip(c, k[2])
        part = span(part, NF)
        return pltpu.make_async_remote_copy(
            src_ref=sf.at[dest(k), i, part], dst_ref=rf.at[k[0], first(cd) * 2 + c, i, part],
            send_sem=s_sem.at[0], recv_sem=rf_sem.at[k[0]],
            device_id=(frag, dev(second(cd), flip(first(cd), k[1]), cd, cd)), device_id_type=MESH)

    def send_s(i, k, part=None):
        cd = flip(c, k[2])
        part = span(part, NS)
        return pltpu.make_async_remote_copy(
            src_ref=ss.at[dest(k), i, part], dst_ref=rs.at[k[1], second(cd) * 2 + c, i, part],
            send_sem=s_sem.at[1], recv_sem=rs_sem.at[k[1]],
            device_id=(frag, dev(flip(second(cd), k[0]), first(cd), cd, cd)), device_id_type=MESH)

    def send_o(k):
        return pltpu.make_async_remote_copy(
            src_ref=sp.at[dest(k), pl.ds(0, rp.shape[1])], dst_ref=rp.at[me],
            send_sem=s_sem.at[2], recv_sem=ro_sem, device_id=(frag, dest(k)), device_id_type=MESH)

    def far_f(k):
        return bool(k[1] or k[2])

    def far_s(k):
        return bool(k[0] or k[2])

    lane = iota((8, 128), 1)

    def put_row(buf, idx, par, g, blocks):
        for t, b in enumerate(blocks):
            buf[idx + (len(blocks) * par + t,)] = g[8 * b:8 * b + 8].astype(BF16)

    def put_ext(buf, idx, g, blocks):
        rolled = []
        for t, b in enumerate(blocks):
            rolled.append(pltpu.roll(g[8 * b:8 * b + 8], (2 * EXT * t - 32) % 128, 1))
        nt = len(blocks)
        for u in range(tiles(nt) - 2 * nt):
            parts = [t for t in range(nt) if 96 * t < 128 * u + 128 and 96 * t + 96 > 128 * u]
            v = rolled[parts[0]]
            for t in parts[1:]:
                v = jnp.where(lane < 96 * t - 128 * u, v, rolled[t])
            buf[idx + (2 * nt + u,)] = v.astype(BF16)

    def places(i, k):
        d = dest(k)
        cd = flip(c, k[2])
        return ((sf, (d, i), range(NF)) if far_f(k) else (rf, (k[0], first(cd) * 2 + c, i), range(NF)),
                (ss, (d, i), range(NF, nb)) if far_s(k) else (rs, (k[1], second(cd) * 2 + c, i), range(NF, nb)))

    zpad = jnp.zeros((8 * n, 128 - n), BF16)
    lane_n = iota((n, 128), 1)

    def wait_row(p):
        row_copy(p).wait()

    def steps12(p, par):
        slot = p % SLOTS
        for g in range(ng):
            a0 = a_buf[slot, 16 * g:16 * g + 8].reshape(8 * n, n)
            a1 = a_buf[slot, 16 * g + 8:16 * g + 16].reshape(8 * n, n)
            w = jnp.concatenate([a0, zpad, a1, zpad], axis=1)
            t = dot(la[...], w)
            for xx in range(no):
                tx = t[8 * xx:8 * xx + 8]
                tx = jnp.concatenate([tx[:, 0:128], tx[:, 128:256]], axis=0).astype(BF16)
                l0 = (xx % 2) * 128
                t_buf[par, xx // 2, 16 * g:16 * g + 16, l0:l0 + 128] = tx
        for e in range(0, nd, 2):
            hh = dot(t_buf[par, e:e + 2].reshape(2 * n, 256), ww[par])
            h_buf[par, e:e + 2] = hh.astype(BF16).reshape(2, n, 256)

    def step3(i, rows):
        for k in KS:
            d = dest(k)
            hs = [h_buf[0, d], h_buf[1, d]]
            e0, e1 = hs[0][:, 128:256], hs[1][:, 128:256]
            cols = [hs[par][:, 0:128] for par in rows]
            if 1 in rows:
                cols.append(jnp.where(lane_n < 80, e0, e1))
            g = dot(cvt_ref[...], jnp.concatenate(cols, axis=1) if len(cols) > 1 else cols[0])
            for buf, idx, blocks in places(i, k):
                for q, par in enumerate(rows):
                    put_row(buf, idx, par, g[:, 128 * q:128 * q + 128], blocks)
                if 1 in rows:
                    put_ext(buf, idx, g[:, 128 * len(rows):], blocks)
            if 1 in rows:
                go = dot_t(jnp.where(lane_n < 32, e0, e1)[:, 0:64], cvs[i]).astype(BF16)
                for u in range(2):
                    sp[d, nv * i // 128 + u] += go[:, 128 * u:128 * u + 128]

    def sends(i, part=None):
        for relayed in (1, 0):
            for k in KS:
                if far_f(k) and k[0] == relayed:
                    send_f(i, k, part).start()
                if far_s(k) and k[1] == relayed:
                    send_s(i, k, part).start()

    def pair(i, _):
        wait_row(2 * i)
        wait_row(2 * i + 1)
        steps12(2 * i, 0)
        steps12(2 * i + 1, 1)
        step3(i, (0, 1))

        sends(i)

        @pl.when(2 * i + SLOTS < np_)
        def _():
            for p in (2 * i + SLOTS, 2 * i + SLOTS + 1):
                row_copy(p).start()

        return 0

    sp[...] = jnp.zeros_like(sp)
    for i in range(npair):
        cvs[i] = dot(cv, onehot(iota((nv, 256), 1) == iota((nv, 256), 0) + nv * i % 128)).astype(BF16)
    wait_row(0)
    steps12(0, 0)
    step3(0, (0,))
    pl.semaphore_wait(barrier, len(NEAR))
    sends(0, 0)
    pl.semaphore_signal(d_sem, inc=1, device_id=(frag, dest((0, 1, 0))), device_id_type=MESH)
    wait_row(1)
    steps12(1, 1)
    step3(0, (1,))
    sends(0, 1)
    for p in (SLOTS, SLOTS + 1):
        row_copy(p).start()

    wait_row(2)
    steps12(2, 0)
    step3(1, (0,))
    sends(1, 0)
    wait_row(3)
    steps12(3, 1)
    step3(1, (1,))
    sends(1, 1)
    for p in (SLOTS + 2, SLOTS + 3):
        row_copy(p).start()

    lax.fori_loop(2, npair, pair, 0)

    pl.semaphore_wait(d_sem, 1)
    nt = rp.shape[1]
    rp[me] = sp[me, 0:nt]
    for k in KS[:-1]:
        send_o(k).start()

    def kron(tab, m_, kk, p_of_col):
        perm = onehot(iota((n, kk), 0) == p_of_col(iota((n, kk), 1)))
        r = onehot(iota((m_ * 8, m_), 0) // 8 == iota((m_ * 8, m_), 1))
        v = dot(r, dot(tab, perm).astype(BF16))
        return jnp.where(iota(v.shape, 0) % 8 == iota(v.shape, 1) % 8, v, 0.0).astype(BF16)

    k4 = npair * 32
    for par in range(2):
        def p_f(t):
            src = t // (8 * npair)
            return np_ * dev(second(c), src // 2, c, src % 2) + 2 * ((t // 8) % npair) + par

        def p_s(t):
            src = t // (8 * npair)
            return np_ * dev(src // 2, first(c), c, src % 2) + 2 * ((t // 8) % npair) + par

        lf[par] = kron(cot_ref[...], no, k4, p_f)
        ls[par] = kron(cot_ref[...], no, k4, p_s)

    def wait_recv(buf, sem):
        pltpu.make_async_remote_copy(
            src_ref=buf, dst_ref=buf, send_sem=s_sem.at[0], recv_sem=sem,
            device_id=(frag, dest((0, 0, 1))), device_id_type=MESH).wait_recv()

    def wait_send(buf, sem):
        pltpu.make_async_remote_copy(
            src_ref=buf, dst_ref=buf, send_sem=sem, recv_sem=ro_sem,
            device_id=(frag, dest((0, 0, 1))), device_id_type=MESH).wait_send()

    lane_k = iota((k4, 128), 1)

    def partial(r, left, w, t, nt):
        def rows(u):
            return r[w, :, :, u].reshape(k4, 128)
        u, off = 96 * t // 128, 96 * t % 128
        e = rows(2 * nt + u)
        if off + 96 > 128:
            e = jnp.where(lane_k >= off, e, rows(2 * nt + u + 1))
        r0 = dot(left[0], jnp.concatenate([rows(t), e], axis=1))
        r1 = dot(left[1], jnp.concatenate([rows(nt + t), e], axis=1))
        main = r0[:, 0:128] + r1[:, 0:128]
        ext = r0[:, 128:256] + pltpu.roll(r1[:, 128:256], 128 - EXT, 1)
        if off:
            ext = pltpu.roll(ext, 128 - off, 1)
        return main.reshape(no, 8, 128), ext.reshape(no, 8, 128)

    def send_p(buf, out, ssem, rsem, h, t):
        return pltpu.make_async_remote_copy(
            src_ref=buf.at[t], dst_ref=out.at[t], send_sem=ssem, recv_sem=rsem.at[t],
            device_id=(frag, dest(h)), device_id_type=MESH)

    F = (rf, lf, pf, qf, p_sem.at[0], qf_sem, (1, 0, 0), NF, 0)
    S = (rs, ls, ps, qs, p_sem.at[1], qs_sem, (0, 1, 0), NS, NF)
    order = [(q, t) for t in range(NF) for q in (F, S) if t < q[7]]

    wait_recv(rf.at[1, pl.ds(0, 3)], rf_sem.at[1])
    wait_recv(rs.at[1, pl.ds(0, 3)], rs_sem.at[1])
    for (r, left, buf, out, ssem, rsem, h, nt, _), t in order:
        main, ext = partial(r, left, 1, t, nt)
        buf[t, 0:no] = main
        for q in range(no // 8):
            row = jnp.concatenate([ext[8 * q + v][:, 0:EXT] for v in range(8)], axis=1)
            for v in range(3):
                buf[t, no + 3 * q + v] = row[:, 128 * v:128 * v + 128]
        send_p(buf, out, ssem, rsem, h, t).start()

    wait_recv(rf.at[0, pl.ds(0, 3)], rf_sem.at[0])
    wait_recv(rs.at[0, pl.ds(0, 3)], rs_sem.at[0])
    for (r, left, _, _, _, _, _, nt, base), t in order:
        main, ext = partial(r, left, 0, t, nt)
        r0 = 8 * (base + t)
        v2_ref[:, r0:r0 + 8, 0:128] = main
        v2_ref[:, r0:r0 + 8, 128:128 + EXT] = ext[:, :, 0:EXT]

    k8 = npair * 128
    l1[...] = kron(cvt_ref[...], nv, k8,
                   lambda t: np_ * (t // (16 * npair)) + 2 * ((t // 16) % npair) + (t // 8) % 2)

    wait_recv(rp.at[pl.ds(0, nd - 1)], ro_sem)

    def unpack(d, _):
        v = jnp.concatenate([rp[d, u] for u in range(rp.shape[1])], axis=1)
        for i in range(npair):
            ro[d, i] = v[:, nv * i:nv * i + nv]
        return 0
    lax.fori_loop(0, nd, unpack, 0)

    for ib in range(4):
        def oo_rows(par):
            return ro[:, :, par * 32 + 8 * ib:par * 32 + 8 * ib + 8].reshape(npair * nd, 8, nv)
        w = jnp.concatenate([oo_rows(0), oo_rows(1)], axis=1).reshape(k8, nv)
        v1_ref[:, 8 * ib:8 * ib + 8, :] = dot(l1[...], w).reshape(nv, 8, nv)

    for (_, _, buf, out, ssem, rsem, h, nt, base), t in order:
        send_p(buf, out, ssem, rsem, h, t).wait_recv()
        r0 = 8 * (base + t)
        v2_ref[:, r0:r0 + 8, 0:128] += out[t, 0:no]
        for q in range(no // 8):
            row = jnp.concatenate([out[t, no + 3 * q + v] for v in range(3)], axis=1)
            for v in range(8):
                v2_ref[8 * q + v, r0:r0 + 8, 128:128 + EXT] += row[:, EXT * v:EXT * v + EXT]

    wait_send(sf.at[pl.ds(0, 6)], s_sem.at[0])
    wait_send(ss.at[pl.ds(0, 6)], s_sem.at[1])
    wait_send(rp.at[pl.ds(0, nd - 1)], s_sem.at[2])
    wait_send(pf, p_sem.at[0])
    wait_send(ps, p_sem.at[1])


def out_kernel(v1_ref, v2_ref, o1_ref, o2_ref, sem):
    cps = []
    for j, (v, o) in enumerate(((v1_ref, o1_ref), (v2_ref, o2_ref))):
        m = v.shape[0] // 4
        for q in range(4):
            cps.append(pltpu.make_async_copy(v.at[pl.ds(m * q, m)], o.at[pl.ds(m * q, m)], sem.at[4 * j + q]))
    for cp in cps:
        cp.start()
    for cp in cps:
        cp.wait()


def solution(mesh):
    nd = mesh.shape["dev"]

    def local_part(a, co, cv):
        np_, n = a.shape[0], a.shape[1]
        no, nv = co.shape[1], cv.shape[1]
        npair, nb = np_ // 2, nv // 8
        ns = nb - NF
        lanes = -(-npair * nv // 128)
        vm = pl.BlockSpec(memory_space=pltpu.VMEM)
        hbm = pl.BlockSpec(memory_space=pltpu.HBM)
        dma = pltpu.SemaphoreType.DMA
        v1, v2 = pl.pallas_call(
            functools.partial(kernel, np_, n, no, nv),
            out_shape=(jax.ShapeDtypeStruct((nv, no * no // nd, nv), F32),
                       jax.ShapeDtypeStruct((no, nv, no * nv // nd), F32)),
            in_specs=[hbm, hbm, hbm],
            out_specs=(vm, vm),
            scratch_shapes=[
                pltpu.VMEM((no, n), BF16),
                pltpu.VMEM((nv, n), BF16),
                pltpu.VMEM((SLOTS, n, n, n), BF16),
                pltpu.VMEM((no * 8, n * 8), BF16),
                pltpu.VMEM((2, 256, 256), BF16),
                pltpu.VMEM((npair, n, 256), BF16),
                pltpu.VMEM((2, nd, n, 256), BF16),
                pltpu.VMEM((2, nd, n, 256), BF16),
                pltpu.VMEM((2, no * 8, npair * 32), BF16),
                pltpu.VMEM((2, no * 8, npair * 32), BF16),
                pltpu.VMEM((nv * 8, npair * 128), BF16),
                pltpu.VMEM((nd, npair, tiles(NF), 8, 128), BF16),
                pltpu.VMEM((nd, npair, tiles(ns), 8, 128), BF16),
                pltpu.VMEM((nd, lanes + 1, 4 * no, 128), BF16),
                pltpu.VMEM((2, 4, npair, tiles(NF), 8, 128), BF16),
                pltpu.VMEM((2, 4, npair, tiles(ns), 8, 128), BF16),
                pltpu.VMEM((nd, lanes, 4 * no, 128), BF16),
                pltpu.VMEM((nd, npair, 4 * no, nv), BF16),
                pltpu.VMEM((NF, no + 3 * no // 8, 8, 128), F32),
                pltpu.VMEM((ns, no + 3 * no // 8, 8, 128), F32),
                pltpu.VMEM((NF, no + 3 * no // 8, 8, 128), F32),
                pltpu.VMEM((ns, no + 3 * no // 8, 8, 128), F32),
                dma((2,)), dma((SLOTS,)), dma((3,)), dma((2,)), dma((2,)), dma,
                dma((2,)), dma((NF,)), dma((ns,)), pltpu.SemaphoreType.REGULAR,
            ],
            compiler_params=pltpu.CompilerParams(
                collective_id=0, has_side_effects=True, vmem_limit_bytes=50 * 1024 * 1024),
        )(a, *(pltpu.with_memory_space_constraint(t.T, pltpu.HBM) for t in (co, cv)))
        hb = pl.BlockSpec(memory_space=pl.ANY)
        v1, v2 = pl.pallas_call(
            out_kernel,
            out_shape=(jax.ShapeDtypeStruct(v1.shape, F32), jax.ShapeDtypeStruct(v2.shape, F32)),
            in_specs=[vm, vm], out_specs=(hb, hb),
            scratch_shapes=[dma((8,))],
            compiler_params=pltpu.CompilerParams(vmem_limit_bytes=4 * 1024 * 1024),
        )(v1, v2)
        return v1.transpose(0, 2, 1), v2

    return jax.shard_map(local_part, mesh=mesh,
                         in_specs=(P(('frag', 'dev')), P('frag'), P('frag')),
                         out_specs=(P('frag', None, 'dev'), P('frag', None, 'dev')),
                         check_vma=False)
```

```python
import functools

import jax
import jax.numpy as jnp
from jax import lax
from jax.experimental import pallas as pl
from jax.experimental.pallas import tpu as pltpu
from jax.sharding import PartitionSpec as P

MESH = pl.DeviceIdType.MESH
F32 = jnp.float32
BF16 = jnp.bfloat16
NF = 6
SLOTS = 6
EXT = 48


def dot(a, b):
    return jnp.dot(a, b, preferred_element_type=F32)


def dot_t(a, b):
    return lax.dot_general(a, b, (((0,), (0,)), ((), ())), preferred_element_type=F32)


def iota(shape, d):
    return lax.broadcasted_iota(jnp.int32, shape, d)


def onehot(cond):
    return jnp.where(cond, 1.0, 0.0).astype(BF16)


def tiles(blocks):
    return 2 * blocks + -(-2 * EXT * blocks // 128)


def kernel(np_, n, no, nv, a_ref, cot_hbm, cvt_hbm, v1_ref, v2_ref,
           cot_ref, cvt_ref, a_buf, la, ww, cvs, t_buf, h_buf, lf, ls, l1,
           sf, ss, sp, rf, rs, rp, ro, pf, ps, qf, qs,
           c_sem, a_sem, s_sem, rf_sem, rs_sem, ro_sem, p_sem, qf_sem, qs_sem, d_sem):
    nd = 8
    npair = np_ // 2
    nb = nv // 8
    NS = nb - NF
    ng = n // 16
    me = lax.axis_index("dev")
    frag = lax.axis_index("frag")
    y, x, c = me // 4, (me // 2) % 2, me % 2

    def first(cd):
        return x + cd * (y - x)

    def second(cd):
        return y + cd * (x - y)

    def dev(s, f, cd, core):
        return (s + cd * (f - s)) * 4 + (f + cd * (s - f)) * 2 + core

    def flip(v, on):
        return 1 - v if on else v

    def dest(k):
        cd = flip(c, k[2])
        return dev(flip(second(cd), k[0]), flip(first(cd), k[1]), cd, cd)

    KS = [(1, 1, 0), (1, 1, 1), (1, 0, 1), (0, 1, 1), (1, 0, 0), (0, 1, 0), (0, 0, 1), (0, 0, 0)]
    NEAR = [k for k in KS[:-1] if not (k[0] and k[1])]

    def row_copy(p):
        return pltpu.make_async_copy(a_ref.at[p], a_buf.at[p % SLOTS], a_sem.at[p % SLOTS])

    CUTS = [0, 4, 7]

    def first_copy(j):
        q = pl.ds(16 * CUTS[j], 16 * (CUTS[j + 1] - CUTS[j]))
        return pltpu.make_async_copy(a_ref.at[0, q], a_buf.at[0, q], c_sem.at[2 + j])

    barrier = pltpu.get_barrier_semaphore()
    for k in NEAR:
        pl.semaphore_signal(barrier, inc=1, device_id=(frag, dest(k)), device_id_type=MESH)
    coefs = [pltpu.make_async_copy(cot_hbm, cot_ref, c_sem.at[0]),
             pltpu.make_async_copy(cvt_hbm, cvt_ref, c_sem.at[1])]
    for cp in coefs:
        cp.start()
    for j in range(len(CUTS) - 1):
        first_copy(j).start()
    for cp in coefs:
        cp.wait()

    cot = cot_ref[...]
    cvt = cvt_ref[...]
    co = dot_t(cot, onehot(iota((no, no), 0) == iota((no, no), 1))).astype(BF16)
    cv = dot_t(cvt, onehot(iota((nv, nv), 0) == iota((nv, nv), 1))).astype(BF16)
    rep8 = onehot(iota((no * 8, no), 0) // 8 == iota((no * 8, no), 1))
    tile = onehot(iota((n, 8 * n), 0) == iota((n, 8 * n), 1) % n)
    m = dot(rep8, dot(cot, tile).astype(BF16))
    la[...] = jnp.where(iota(m.shape, 0) % 8 == iota(m.shape, 1) // n, m, 0.0).astype(BF16)
    row_copy(1).start()
    ww[...] = jnp.zeros_like(ww)
    for par in range(2):
        for j in range(2):
            jb = iota((nv, 256), 0) + j * nv
            sel_v = onehot(iota((nv, 256), 1) == jnp.where(jb < 128, jb, jb + 32 + EXT * par))
            sel_o = onehot(iota((no, 256), 1) == iota((no, 256), 0) + 128 + 32 * par + no * j)
            ww[par, 128 * j:128 * j + n, :] = (dot(cv, sel_v) + dot(co, sel_o)).astype(BF16)

    for p in range(2, SLOTS):
        row_copy(p).start()

    def span(part, nt):
        return {None: pl.ds(0, tiles(nt)), 0: pl.ds(0, nt), 1: pl.ds(nt, tiles(nt) - nt)}[part]

    def send_f(i, k, part=None):
        cd = flip(c, k[2])
        part = span(part, NF)
        return pltpu.make_async_remote_copy(
            src_ref=sf.at[dest(k), i, part], dst_ref=rf.at[k[0], first(cd) * 2 + c, i, part],
            send_sem=s_sem.at[0], recv_sem=rf_sem.at[k[0]],
            device_id=(frag, dev(second(cd), flip(first(cd), k[1]), cd, cd)), device_id_type=MESH)

    def send_s(i, k, part=None):
        cd = flip(c, k[2])
        part = span(part, NS)
        return pltpu.make_async_remote_copy(
            src_ref=ss.at[dest(k), i, part], dst_ref=rs.at[k[1], second(cd) * 2 + c, i, part],
            send_sem=s_sem.at[1], recv_sem=rs_sem.at[k[1]],
            device_id=(frag, dev(flip(second(cd), k[0]), first(cd), cd, cd)), device_id_type=MESH)

    def send_o(k):
        return pltpu.make_async_remote_copy(
            src_ref=sp.at[dest(k), pl.ds(0, rp.shape[1])], dst_ref=rp.at[me],
            send_sem=s_sem.at[2], recv_sem=ro_sem, device_id=(frag, dest(k)), device_id_type=MESH)

    def far_f(k):
        return bool(k[1] or k[2])

    def far_s(k):
        return bool(k[0] or k[2])

    lane = iota((8, 128), 1)

    def put_row(buf, idx, par, g, blocks):
        for t, b in enumerate(blocks):
            buf[idx + (len(blocks) * par + t,)] = g[8 * b:8 * b + 8].astype(BF16)

    def put_ext(buf, idx, g, blocks):
        rolled = []
        for t, b in enumerate(blocks):
            rolled.append(pltpu.roll(g[8 * b:8 * b + 8], (2 * EXT * t - 32) % 128, 1))
        nt = len(blocks)
        for u in range(tiles(nt) - 2 * nt):
            parts = [t for t in range(nt) if 96 * t < 128 * u + 128 and 96 * t + 96 > 128 * u]
            v = rolled[parts[0]]
            for t in parts[1:]:
                v = jnp.where(lane < 96 * t - 128 * u, v, rolled[t])
            buf[idx + (2 * nt + u,)] = v.astype(BF16)

    def places(i, k):
        d = dest(k)
        cd = flip(c, k[2])
        return ((sf, (d, i), range(NF)) if far_f(k) else (rf, (k[0], first(cd) * 2 + c, i), range(NF)),
                (ss, (d, i), range(NF, nb)) if far_s(k) else (rs, (k[1], second(cd) * 2 + c, i), range(NF, nb)))

    zpad = jnp.zeros((8 * n, 128 - n), BF16)
    lane_n = iota((n, 128), 1)

    def wait_row(p):
        row_copy(p).wait()

    def steps12(p, par, chunks=False):
        slot = p % SLOTS
        for g in range(ng):
            if chunks and g in CUTS:
                first_copy(CUTS.index(g)).wait()
            a0 = a_buf[slot, 16 * g:16 * g + 8].reshape(8 * n, n)
            a1 = a_buf[slot, 16 * g + 8:16 * g + 16].reshape(8 * n, n)
            w = jnp.concatenate([a0, zpad, a1, zpad], axis=1)
            t = dot(la[...], w)
            for xx in range(no):
                tx = t[8 * xx:8 * xx + 8]
                tx = jnp.concatenate([tx[:, 0:128], tx[:, 128:256]], axis=0).astype(BF16)
                l0 = (xx % 2) * 128
                t_buf[par, xx // 2, 16 * g:16 * g + 16, l0:l0 + 128] = tx
        for e in range(0, nd, 2):
            hh = dot(t_buf[par, e:e + 2].reshape(2 * n, 256), ww[par])
            h_buf[par, e:e + 2] = hh.astype(BF16).reshape(2, n, 256)

    def step3(i, rows):
        for k in KS:
            d = dest(k)
            hs = [h_buf[0, d], h_buf[1, d]]
            e0, e1 = hs[0][:, 128:256], hs[1][:, 128:256]
            cols = [hs[par][:, 0:128] for par in rows]
            if 1 in rows:
                cols.append(jnp.where(lane_n < 80, e0, e1))
            g = dot(cvt_ref[...], jnp.concatenate(cols, axis=1) if len(cols) > 1 else cols[0])
            for buf, idx, blocks in places(i, k):
                for q, par in enumerate(rows):
                    put_row(buf, idx, par, g[:, 128 * q:128 * q + 128], blocks)
                if 1 in rows:
                    put_ext(buf, idx, g[:, 128 * len(rows):], blocks)
            if 1 in rows:
                go = dot_t(jnp.where(lane_n < 32, e0, e1)[:, 0:64], cvs[i]).astype(BF16)
                for u in range(2):
                    sp[d, nv * i // 128 + u] += go[:, 128 * u:128 * u + 128]

    def sends(i, part=None):
        for relayed in (1, 0):
            for k in KS:
                if far_f(k) and k[0] == relayed:
                    send_f(i, k, part).start()
                if far_s(k) and k[1] == relayed:
                    send_s(i, k, part).start()

    def pair(i, _):
        wait_row(2 * i)
        wait_row(2 * i + 1)
        steps12(2 * i, 0)
        steps12(2 * i + 1, 1)
        step3(i, (0, 1))

        sends(i)

        @pl.when(2 * i + SLOTS < np_)
        def _():
            for p in (2 * i + SLOTS, 2 * i + SLOTS + 1):
                row_copy(p).start()

        return 0

    sp[...] = jnp.zeros_like(sp)
    for i in range(npair):
        cvs[i] = dot(cv, onehot(iota((nv, 256), 1) == iota((nv, 256), 0) + nv * i % 128)).astype(BF16)
    steps12(0, 0, True)
    step3(0, (0,))
    pl.semaphore_wait(barrier, len(NEAR))
    sends(0, 0)
    pl.semaphore_signal(d_sem, inc=1, device_id=(frag, dest((0, 1, 0))), device_id_type=MESH)
    wait_row(1)
    steps12(1, 1)
    step3(0, (1,))
    sends(0, 1)
    for p in (SLOTS, SLOTS + 1):
        row_copy(p).start()

    wait_row(2)
    steps12(2, 0)
    step3(1, (0,))
    sends(1, 0)
    wait_row(3)
    steps12(3, 1)
    step3(1, (1,))
    sends(1, 1)
    for p in (SLOTS + 2, SLOTS + 3):
        row_copy(p).start()

    lax.fori_loop(2, npair, pair, 0)

    pl.semaphore_wait(d_sem, 1)
    nt = rp.shape[1]
    rp[me] = sp[me, 0:nt]
    for k in KS[:-1]:
        send_o(k).start()

    def kron(tab, m_, kk, p_of_col):
        perm = onehot(iota((n, kk), 0) == p_of_col(iota((n, kk), 1)))
        r = onehot(iota((m_ * 8, m_), 0) // 8 == iota((m_ * 8, m_), 1))
        v = dot(r, dot(tab, perm).astype(BF16))
        return jnp.where(iota(v.shape, 0) % 8 == iota(v.shape, 1) % 8, v, 0.0).astype(BF16)

    k4 = npair * 32
    for par in range(2):
        def p_f(t):
            src = t // (8 * npair)
            return np_ * dev(second(c), src // 2, c, src % 2) + 2 * ((t // 8) % npair) + par

        def p_s(t):
            src = t // (8 * npair)
            return np_ * dev(src // 2, first(c), c, src % 2) + 2 * ((t // 8) % npair) + par

        lf[par] = kron(cot_ref[...], no, k4, p_f)
        ls[par] = kron(cot_ref[...], no, k4, p_s)

    def wait_recv(buf, sem):
        pltpu.make_async_remote_copy(
            src_ref=buf, dst_ref=buf, send_sem=s_sem.at[0], recv_sem=sem,
            device_id=(frag, dest((0, 0, 1))), device_id_type=MESH).wait_recv()

    def wait_send(buf, sem):
        pltpu.make_async_remote_copy(
            src_ref=buf, dst_ref=buf, send_sem=sem, recv_sem=ro_sem,
            device_id=(frag, dest((0, 0, 1))), device_id_type=MESH).wait_send()

    lane_k = iota((k4, 128), 1)

    def partial(r, left, w, t, nt):
        def rows(u):
            return r[w, :, :, u].reshape(k4, 128)
        u, off = 96 * t // 128, 96 * t % 128
        e = rows(2 * nt + u)
        if off + 96 > 128:
            e = jnp.where(lane_k >= off, e, rows(2 * nt + u + 1))
        r0 = dot(left[0], jnp.concatenate([rows(t), e], axis=1))
        r1 = dot(left[1], jnp.concatenate([rows(nt + t), e], axis=1))
        main = r0[:, 0:128] + r1[:, 0:128]
        ext = r0[:, 128:256] + pltpu.roll(r1[:, 128:256], 128 - EXT, 1)
        if off:
            ext = pltpu.roll(ext, 128 - off, 1)
        return main.reshape(no, 8, 128), ext.reshape(no, 8, 128)

    def send_p(buf, out, ssem, rsem, h, t):
        return pltpu.make_async_remote_copy(
            src_ref=buf.at[t], dst_ref=out.at[t], send_sem=ssem, recv_sem=rsem.at[t],
            device_id=(frag, dest(h)), device_id_type=MESH)

    F = (rf, lf, pf, qf, p_sem.at[0], qf_sem, (1, 0, 0), NF, 0)
    S = (rs, ls, ps, qs, p_sem.at[1], qs_sem, (0, 1, 0), NS, NF)
    order = [(q, t) for t in range(NF) for q in (F, S) if t < q[7]]

    wait_recv(rf.at[1, pl.ds(0, 3)], rf_sem.at[1])
    wait_recv(rs.at[1, pl.ds(0, 3)], rs_sem.at[1])
    for (r, left, buf, out, ssem, rsem, h, nt, _), t in order:
        main, ext = partial(r, left, 1, t, nt)
        buf[t, 0:no] = main
        for q in range(no // 8):
            row = jnp.concatenate([ext[8 * q + v][:, 0:EXT] for v in range(8)], axis=1)
            for v in range(3):
                buf[t, no + 3 * q + v] = row[:, 128 * v:128 * v + 128]
        send_p(buf, out, ssem, rsem, h, t).start()

    wait_recv(rf.at[0, pl.ds(0, 3)], rf_sem.at[0])
    wait_recv(rs.at[0, pl.ds(0, 3)], rs_sem.at[0])
    for (r, left, _, _, _, _, _, nt, base), t in order:
        main, ext = partial(r, left, 0, t, nt)
        r0 = 8 * (base + t)
        v2_ref[:, r0:r0 + 8, 0:128] = main
        v2_ref[:, r0:r0 + 8, 128:128 + EXT] = ext[:, :, 0:EXT]

    k8 = npair * 128
    l1[...] = kron(cvt_ref[...], nv, k8,
                   lambda t: np_ * (t // (16 * npair)) + 2 * ((t // 16) % npair) + (t // 8) % 2)

    wait_recv(rp.at[pl.ds(0, nd - 1)], ro_sem)

    def unpack(d, _):
        v = jnp.concatenate([rp[d, u] for u in range(rp.shape[1])], axis=1)
        for i in range(npair):
            ro[d, i] = v[:, nv * i:nv * i + nv]
        return 0
    lax.fori_loop(0, nd, unpack, 0)

    for ib in range(4):
        def oo_rows(par):
            return ro[:, :, par * 32 + 8 * ib:par * 32 + 8 * ib + 8].reshape(npair * nd, 8, nv)
        w = jnp.concatenate([oo_rows(0), oo_rows(1)], axis=1).reshape(k8, nv)
        v1_ref[:, 8 * ib:8 * ib + 8, :] = dot(l1[...], w).reshape(nv, 8, nv)

    for (_, _, buf, out, ssem, rsem, h, nt, base), t in order:
        send_p(buf, out, ssem, rsem, h, t).wait_recv()
        r0 = 8 * (base + t)
        v2_ref[:, r0:r0 + 8, 0:128] += out[t, 0:no]
        for q in range(no // 8):
            row = jnp.concatenate([out[t, no + 3 * q + v] for v in range(3)], axis=1)
            for v in range(8):
                v2_ref[8 * q + v, r0:r0 + 8, 128:128 + EXT] += row[:, EXT * v:EXT * v + EXT]

    wait_send(sf.at[pl.ds(0, 6)], s_sem.at[0])
    wait_send(ss.at[pl.ds(0, 6)], s_sem.at[1])
    wait_send(rp.at[pl.ds(0, nd - 1)], s_sem.at[2])
    wait_send(pf, p_sem.at[0])
    wait_send(ps, p_sem.at[1])


def out_kernel(v1_ref, v2_ref, o1_ref, o2_ref, sem):
    cps = []
    for j, (v, o) in enumerate(((v1_ref, o1_ref), (v2_ref, o2_ref))):
        m = v.shape[0] // 4
        for q in range(4):
            cps.append(pltpu.make_async_copy(v.at[pl.ds(m * q, m)], o.at[pl.ds(m * q, m)], sem.at[4 * j + q]))
    for cp in cps:
        cp.start()
    for cp in cps:
        cp.wait()


def solution(mesh):
    nd = mesh.shape["dev"]

    def local_part(a, co, cv):
        np_, n = a.shape[0], a.shape[1]
        no, nv = co.shape[1], cv.shape[1]
        npair, nb = np_ // 2, nv // 8
        ns = nb - NF
        lanes = -(-npair * nv // 128)
        vm = pl.BlockSpec(memory_space=pltpu.VMEM)
        hbm = pl.BlockSpec(memory_space=pltpu.HBM)
        dma = pltpu.SemaphoreType.DMA
        v1, v2 = pl.pallas_call(
            functools.partial(kernel, np_, n, no, nv),
            out_shape=(jax.ShapeDtypeStruct((nv, no * no // nd, nv), F32),
                       jax.ShapeDtypeStruct((no, nv, no * nv // nd), F32)),
            in_specs=[hbm, hbm, hbm],
            out_specs=(vm, vm),
            scratch_shapes=[
                pltpu.VMEM((no, n), BF16),
                pltpu.VMEM((nv, n), BF16),
                pltpu.VMEM((SLOTS, n, n, n), BF16),
                pltpu.VMEM((no * 8, n * 8), BF16),
                pltpu.VMEM((2, 256, 256), BF16),
                pltpu.VMEM((npair, n, 256), BF16),
                pltpu.VMEM((2, nd, n, 256), BF16),
                pltpu.VMEM((2, nd, n, 256), BF16),
                pltpu.VMEM((2, no * 8, npair * 32), BF16),
                pltpu.VMEM((2, no * 8, npair * 32), BF16),
                pltpu.VMEM((nv * 8, npair * 128), BF16),
                pltpu.VMEM((nd, npair, tiles(NF), 8, 128), BF16),
                pltpu.VMEM((nd, npair, tiles(ns), 8, 128), BF16),
                pltpu.VMEM((nd, lanes + 1, 4 * no, 128), BF16),
                pltpu.VMEM((2, 4, npair, tiles(NF), 8, 128), BF16),
                pltpu.VMEM((2, 4, npair, tiles(ns), 8, 128), BF16),
                pltpu.VMEM((nd, lanes, 4 * no, 128), BF16),
                pltpu.VMEM((nd, npair, 4 * no, nv), BF16),
                pltpu.VMEM((NF, no + 3 * no // 8, 8, 128), F32),
                pltpu.VMEM((ns, no + 3 * no // 8, 8, 128), F32),
                pltpu.VMEM((NF, no + 3 * no // 8, 8, 128), F32),
                pltpu.VMEM((ns, no + 3 * no // 8, 8, 128), F32),
                dma((4,)), dma((SLOTS,)), dma((3,)), dma((2,)), dma((2,)), dma,
                dma((2,)), dma((NF,)), dma((ns,)), pltpu.SemaphoreType.REGULAR,
            ],
            compiler_params=pltpu.CompilerParams(
                collective_id=0, has_side_effects=True, vmem_limit_bytes=50 * 1024 * 1024),
        )(a, *(pltpu.with_memory_space_constraint(t.T, pltpu.HBM) for t in (co, cv)))
        hb = pl.BlockSpec(memory_space=pl.ANY)
        v1, v2 = pl.pallas_call(
            out_kernel,
            out_shape=(jax.ShapeDtypeStruct(v1.shape, F32), jax.ShapeDtypeStruct(v2.shape, F32)),
            in_specs=[vm, vm], out_specs=(hb, hb),
            scratch_shapes=[dma((8,))],
            compiler_params=pltpu.CompilerParams(vmem_limit_bytes=4 * 1024 * 1024),
        )(v1, v2)
        return v1.transpose(0, 2, 1), v2

    return jax.shard_map(local_part, mesh=mesh,
                         in_specs=(P(('frag', 'dev')), P('frag'), P('frag')),
                         out_specs=(P('frag', None, 'dev'), P('frag', None, 'dev')),
                         check_vma=False)
```
